32 devices in a mesh: data: 2 (over x), pp: 4 (over z), ep: 4 (over y, core).
Axes of the slice: x: 2, y: 2, z: 4, core: 2. Of those that a mesh axis runs over, the one named last changes fastest.
Arguments:
- expert_out: bfloat16 [8, 1, 128, 32, 4096], P(('data', 'pp'), None, 'ep'), parts along dimension 0
- expert_id: int32 [8, 1, 256, 8], P(('data', 'pp'), None, 'ep'), parts along dimension 0
- slot_id: int32 [8, 1, 256, 8], P(('data', 'pp'), None, 'ep'), parts along dimension 0
- gate: float32 [8, 1, 256, 8], P(('data', 'pp'), None, 'ep'), parts along dimension 0
- resid: bfloat16 [8, 1, 256, 4096], P(('data', 'pp'), None, 'ep'), parts along dimension 0
- owner: int32 [8, 32], P(('data', 'pp')), parts along dimension 0
- norm_w: float32 [4, 4096], P('pp')
- w_q: bfloat16 [4, 4096, 8192], P('pp')
- w_k: bfloat16 [4, 4096, 8192], P('pp')
- w_v: bfloat16 [4, 4096, 8192], P('pp')
- w_o: bfloat16 [4, 8192, 4096], P('pp')
Outputs:
- output: bfloat16 [8, 1, 256, 4096], P(('data', 'pp'), None, 'ep'), parts along dimension 0
There are 2 independent parts. The reference program is written for one: setup_inputs(seed, part) draws one part's arguments, and reference() takes and returns one part's arrays. A program takes and returns all parts, laid end to end along the dimension named above; an argument that names none is the same for every part.
All inputs are finite; a program needn't handle non-finite values.
Results may differ from the reference program's by a relative error of at most 0.013572.
Values are sent between devices in bfloat16 or wider.
A program may use at most 1.25 GiB of HBM per device.

```python
import jax
import jax.numpy as jnp
from jax import lax

STAGES = 4
EP_DEVICES = 4
MICRO = 1
SEQ_DEV = 8
SEQ_LEN = 8
MODEL_DIM = 4096
EXPERTS = 128
TOP_K = 8
HEADS = 64
HEAD_DIM = 128
CAP_DEV = 8

SEQS = EP_DEVICES * SEQ_DEV
TOKENS = SEQS * SEQ_LEN
TOK_DEV = SEQ_DEV * SEQ_LEN
CAPACITY = EP_DEVICES * CAP_DEV
QKV_WIDTH = HEADS * HEAD_DIM
HOT_COUNT = max(1, EXPERTS // 32)
HOT_BIAS = (2000 * TOP_K) // EXPERTS
NORM_EPS = 1e-6


def draw_routing(rng_key):
    key_hot, key_score = jax.random.split(rng_key)
    hot_rank = jax.random.permutation(key_hot, EXPERTS)
    hot_bias = jnp.where(hot_rank < HOT_COUNT, HOT_BIAS, 0)
    rand_score = jax.random.randint(key_score, (STAGES, MICRO, EP_DEVICES, TOK_DEV, EXPERTS), 0, 1000)
    tok_local = jnp.arange(TOK_DEV)[:, None]
    forced = jnp.where((tok_local < CAP_DEV) & (hot_rank[None, :] == 0), 4000, 0)
    full_score = (rand_score + hot_bias + forced) * EXPERTS + jnp.arange(EXPERTS)
    chosen = lax.top_k(full_score, TOP_K)[1].astype(jnp.int32)
    n_flat = TOK_DEV * TOP_K
    flat_ids = chosen.reshape(STAGES, MICRO, EP_DEVICES, n_flat)
    flat_pos = jnp.arange(n_flat)
    sort_order = jnp.argsort(flat_ids * n_flat + flat_pos, axis=-1)
    sorted_ids = jnp.take_along_axis(flat_ids, sort_order, axis=-1)
    prev_ids = jnp.concatenate([jnp.full_like(sorted_ids[..., :1], -1), sorted_ids[..., :-1]], axis=-1)
    group_start = lax.cummax(jnp.where(sorted_ids != prev_ids, flat_pos, 0), axis=3)
    rank_sorted = flat_pos - group_start
    slot_pos = jnp.take_along_axis(rank_sorted, jnp.argsort(sort_order, axis=-1), axis=-1)
    dev_base = (jnp.arange(EP_DEVICES) * CAP_DEV)[:, None]
    slot_all = jnp.where(slot_pos < CAP_DEV, dev_base + slot_pos, -1).astype(jnp.int32)
    return chosen.reshape(STAGES, MICRO, TOKENS, TOP_K), slot_all.reshape(STAGES, MICRO, TOKENS, TOP_K)


def draw_owner(rng_key):
    key_src, key_dst = jax.random.split(rng_key)
    seq_rows = jnp.broadcast_to(jnp.arange(SEQ_DEV), (STAGES, EP_DEVICES, SEQ_DEV))
    local_perm = jax.random.permutation(key_src, seq_rows, axis=2, independent=True)
    global_ids = local_perm + (jnp.arange(EP_DEVICES) * SEQ_DEV)[:, None]
    per_pair = SEQ_DEV // EP_DEVICES
    global_ids = global_ids.reshape(STAGES, EP_DEVICES, EP_DEVICES, per_pair).transpose(0, 2, 1, 3).reshape(STAGES, EP_DEVICES, SEQ_DEV)
    shuffle = jax.random.permutation(key_dst, seq_rows, axis=2, independent=True)
    owned = jnp.take_along_axis(global_ids, shuffle, axis=2)
    return owned.reshape(STAGES, SEQS).astype(jnp.int32)


def setup_inputs(seed: int = 0, part: int = 0) -> dict:
    part_key = jax.random.fold_in(jax.random.key(seed), part)
    keys_data = jax.random.split(part_key, 8)
    keys_weight = jax.random.split(jax.random.key(seed + 1), 6)
    expert_id, slot_id = draw_routing(keys_data[0])
    owner = draw_owner(keys_data[1])
    expert_scale = jnp.exp(0.7 * jax.random.normal(keys_data[2], (STAGES, MICRO, EXPERTS, 1, 1), jnp.float32))
    expert_out = (jax.random.normal(keys_data[3], (STAGES, MICRO, EXPERTS, CAPACITY, MODEL_DIM), jnp.float32) * expert_scale).astype(jnp.bfloat16)
    gate_raw = jnp.exp(1.2 * jax.random.normal(keys_data[4], (STAGES, MICRO, TOKENS, TOP_K), jnp.float32))
    gate_level = 0.5 + jax.random.uniform(keys_data[5], (STAGES, MICRO, TOKENS, 1), jnp.float32)
    gate = gate_raw / jnp.sum(gate_raw, axis=-1, keepdims=True) * gate_level
    resid = jax.random.normal(keys_data[6], (STAGES, MICRO, TOKENS, MODEL_DIM), jnp.float32).astype(jnp.bfloat16)
    norm_w = jax.random.uniform(keys_weight[0], (STAGES, MODEL_DIM), jnp.float32, 0.5, 1.5)
    qk_scale = 1.5 * MODEL_DIM ** -0.5
    w_q = (jax.random.normal(keys_weight[1], (STAGES, MODEL_DIM, QKV_WIDTH), jnp.float32) * qk_scale).astype(jnp.bfloat16)
    w_k = (jax.random.normal(keys_weight[2], (STAGES, MODEL_DIM, QKV_WIDTH), jnp.float32) * qk_scale).astype(jnp.bfloat16)
    w_v = (jax.random.normal(keys_weight[3], (STAGES, MODEL_DIM, QKV_WIDTH), jnp.float32) * MODEL_DIM ** -0.5).astype(jnp.bfloat16)
    w_o = (jax.random.normal(keys_weight[4], (STAGES, QKV_WIDTH, MODEL_DIM), jnp.float32) * QKV_WIDTH ** -0.5).astype(jnp.bfloat16)
    return dict(expert_out=expert_out, expert_id=expert_id, slot_id=slot_id, gate=gate, resid=resid, owner=owner, norm_w=norm_w, w_q=w_q, w_k=w_k, w_v=w_v, w_o=w_o)


def attend_block(y_seq, norm_scale, w_q_stage, w_k_stage, w_v_stage, w_o_stage):
    y_f32 = y_seq.astype(jnp.float32)
    inv_rms = lax.rsqrt(jnp.mean(y_f32 * y_f32, axis=-1, keepdims=True) + NORM_EPS)
    normed = (y_f32 * inv_rms * norm_scale).astype(jnp.bfloat16)
    queries = jnp.dot(normed, w_q_stage, preferred_element_type=jnp.float32).astype(jnp.bfloat16).reshape(SEQ_LEN, HEADS, HEAD_DIM)
    key_vecs = jnp.dot(normed, w_k_stage, preferred_element_type=jnp.float32).astype(jnp.bfloat16).reshape(SEQ_LEN, HEADS, HEAD_DIM)
    values = jnp.dot(normed, w_v_stage, preferred_element_type=jnp.float32).astype(jnp.bfloat16).reshape(SEQ_LEN, HEADS, HEAD_DIM)
    scores = jnp.einsum('qhe,khe->hqk', queries.astype(jnp.float32), key_vecs.astype(jnp.float32)) * HEAD_DIM ** -0.5
    causal = jnp.arange(SEQ_LEN)[:, None] >= jnp.arange(SEQ_LEN)[None, :]
    attn_probs = jax.nn.softmax(jnp.where(causal, scores, -1e30), axis=-1).astype(jnp.bfloat16)
    head_mix = jnp.einsum('hqk,khe->qhe', attn_probs.astype(jnp.float32), values.astype(jnp.float32)).astype(jnp.bfloat16).reshape(SEQ_LEN, QKV_WIDTH)
    out_proj = jnp.dot(head_mix, w_o_stage, preferred_element_type=jnp.float32).astype(jnp.bfloat16)
    return (y_f32 + out_proj.astype(jnp.float32)).astype(jnp.bfloat16)


def reference(expert_out, expert_id, slot_id, gate, resid, owner, norm_w, w_q, w_k, w_v, w_o):
    from_prev = tuple(jnp.roll(arr_in, 1, axis=0) for arr_in in (expert_out, expert_id, slot_id, gate, resid))

    def per_stage(stage_args):
        out_s, ids_s, slots_s, gate_s, resid_s, owner_s, norm_s, w_q_s, w_k_s, w_v_s, w_o_s = stage_args

        def per_micro(micro_args):
            out_m, ids_m, slots_m, gate_m, resid_m = micro_args
            flat_out = out_m.reshape(EXPERTS * CAPACITY, MODEL_DIM)

            def per_seq(seq_index):
                seq_start = seq_index * SEQ_LEN
                ids_q = lax.dynamic_slice_in_dim(ids_m, seq_start, SEQ_LEN, 0)
                slots_q = lax.dynamic_slice_in_dim(slots_m, seq_start, SEQ_LEN, 0)
                gate_q = lax.dynamic_slice_in_dim(gate_m, seq_start, SEQ_LEN, 0)
                resid_q = lax.dynamic_slice_in_dim(resid_m, seq_start, SEQ_LEN, 0)
                kept_mask = slots_q >= 0
                row_index = ids_q * CAPACITY + jnp.where(kept_mask, slots_q, 0)
                picked = flat_out[row_index].astype(jnp.float32)
                weights = jnp.where(kept_mask, gate_q, 0.0)
                combined = jnp.einsum('lk,lkd->ld', weights, picked)
                y_seq = (resid_q.astype(jnp.float32) + combined).astype(jnp.bfloat16)
                return attend_block(y_seq, norm_s, w_q_s, w_k_s, w_v_s, w_o_s)

            return lax.map(per_seq, owner_s)

        return lax.map(per_micro, (out_s, ids_s, slots_s, gate_s, resid_s))

    result = lax.map(per_stage, from_prev + (owner, norm_w, w_q, w_k, w_v, w_o))
    return result.reshape(STAGES, MICRO, TOKENS, MODEL_DIM)
```

```python
import functools

import jax
import jax.numpy as jnp
from jax import lax
from jax.experimental import pallas as pl
from jax.experimental.pallas import tpu as pltpu
from jax.sharding import PartitionSpec as P

HEAD_DIM = 128
NORM_EPS = 1e-6
SEQ = 8
N_EP = 4
SLOTS = 24
RING_GROUPS = 4
ROWS = 32
PIECE = 16
LANES = 128
BF16_MAX = 3.3895314e38
MESH_ID = pl.DeviceIdType.MESH
F32 = jnp.float32
BF16 = jnp.bfloat16


def mm(a, b):
    return jnp.dot(a, b, preferred_element_type=F32)


def mm_t(a, b):
    return lax.dot_general(a, b, (((1,), (1,)), ((), ())), preferred_element_type=F32)


def split3(x):
    hi = jnp.clip(x, -BF16_MAX, BF16_MAX).astype(BF16)
    r1 = x - hi.astype(F32)
    mid = r1.astype(BF16)
    lo = (r1 - mid.astype(F32)).astype(BF16)
    return hi, mid, lo


def stage_kernel(
    n_pp, gw, exp_rows,
    meta_ref, own_ref, nw_ref, o_hbm, h_hbm, wq_hbm, wk_hbm, wv_hbm, wo_hbm,
    z_hbm,
    wbuf, pbuf, precv, yrecv, zsend, ybuf, xbuf, qkv, abuf, zbuf, hbuf, gbuf, metas, ownr, tok, mp,
    wsem, osem, hsem, msend, mrecv, osend, orecv, psend, prcv, ysend, yrcv, zsnd, zrcv, fsend, frcv, asend, arcv,
    outl, outs, outr,
):
    d_model = nw_ref.shape[1]
    half = d_model // 2
    e_half = wq_hbm.shape[1] // 2
    n_grp = e_half // gw
    slot_rows = wbuf.shape[1]
    n_out = half // gw
    grp_per_slot = slot_rows // gw
    tok_chip = 2 * 8 * SEQ
    tok_dev = 8 * SEQ
    n_chunk = tok_chip // ROWS
    n_piece = tok_chip // PIECE

    me = lax.axis_index("ep")
    core = lax.rem(me, 2)
    chip = me // 2
    partner = chip * 2 + (1 - core)
    across = (1 - chip) * 2 + core
    rank = lax.axis_index("pp")
    nxt = lax.rem(rank + 1, n_pp)
    prv = lax.rem(rank + n_pp - 1, n_pp)

    def remote(src, dst, s_sem, r_sem, dev):
        return pltpu.make_async_remote_copy(
            src_ref=src, dst_ref=dst, send_sem=s_sem, recv_sem=r_sem, device_id=dev, device_id_type=MESH_ID)

    def qkv_copy(mat, kh, g, slot):
        src = (wq_hbm, wk_hbm, wv_hbm)[mat]
        cols = pl.ds(pl.multiple_of(core * e_half + g * gw, gw), gw)
        return pltpu.make_async_copy(
            src.at[pl.ds(kh * slot_rows, slot_rows), cols], wbuf.at[slot], wsem.at[slot])

    def wo_copy(w):
        n, kq = w // 4, lax.rem(w, 4)
        rows = pl.ds(pl.multiple_of(kq * slot_rows, slot_rows), slot_rows)
        cols = pl.ds(pl.multiple_of(core * half + n * gw, gw), gw)
        slot = lax.rem(6 * n_grp + w, SLOTS)
        return pltpu.make_async_copy(wo_hbm.at[rows, cols], wbuf.at[slot], wsem.at[slot])

    o_slot = SLOTS - 4

    def o_copy(nb):
        return pltpu.make_async_copy(
            o_hbm.at[:, pl.ds(nb * gw, gw)],
            wbuf.at[o_slot + nb // 2, pl.ds((nb % 2) * exp_rows, exp_rows)], osem.at[nb])

    h_copy = pltpu.make_async_copy(h_hbm, hbuf, hsem)
    for nb in range(8):
        o_copy(nb).start()
    h_copy.start()
    first = [(g, j) for g in range(RING_GROUPS) for j in range(6)]
    for t, (g, j) in enumerate(first[:o_slot]):
        qkv_copy(j // 2, j % 2, g, t).start()

    barrier = pltpu.get_barrier_semaphore()
    for off in (1, 2, 3):
        pl.semaphore_signal(barrier, inc=1, device_id={"ep": lax.rem(me + off, N_EP)}, device_id_type=MESH_ID)
    pl.semaphore_signal(barrier, inc=1, device_id={"pp": nxt}, device_id_type=MESH_ID)
    pl.semaphore_signal(barrier, inc=1, device_id={"pp": prv}, device_id_type=MESH_ID)
    pl.semaphore_wait(barrier, 5)

    own_copy = remote(own_ref, ownr, osend, orecv, {"pp": prv})
    own_copy.start()
    meta_copies = [
        remote(meta_ref, metas.at[me], msend.at[off - 1], mrecv.at[off - 1], {"ep": lax.rem(me + off, N_EP)})
        for off in (1, 2, 3)]
    for cp in meta_copies:
        cp.start()
    metas[me] = meta_ref[...]
    own_copy.wait_recv()
    sub = lax.broadcasted_iota(jnp.int32, (SEQ, LANES), 0).astype(F32)
    for b in range(4 * SEQ):
        row = jnp.broadcast_to(ownr[b:b + 1, :], (SEQ, LANES))
        tok[b * SEQ:(b + 1) * SEQ, :] = row * float(SEQ) + sub
    for cp in meta_copies:
        cp.wait_recv()
    lane = lax.broadcasted_iota(jnp.int32, (4 * tok_dev, LANES), 1).astype(F32)
    routed = None
    for d in range(N_EP):
        hit = (tok[...] - float(d * tok_dev) == lane) & (lane < float(tok_dev))
        perm = jnp.where(hit, 1.0, 0.0).astype(BF16)
        parts = jnp.concatenate(split3(metas[d]), axis=0)
        term = mm_t(perm, parts)
        routed = term if routed is None else routed + term
    mp[:, 0:48] = routed

    for nb in range(8):
        o_copy(nb).wait()
    h_copy.wait()

    def pair_copy(s, row0):
        rows = pl.ds(row0, ROWS)
        return remote(pbuf.at[1 - core, rows], precv.at[rows], psend.at[s], prcv.at[s], {"ep": partner})

    def y_copy(k):
        src = pl.ds(pl.multiple_of((1 - chip) * tok_chip + k * PIECE, PIECE), PIECE)
        dst = pl.ds(pl.multiple_of(k * PIECE, PIECE), PIECE)
        return remote(pbuf.at[core, src], yrecv.at[dst], ysend.at[k], yrcv.at[k], {"ep": across})

    def chunk_row(s):
        blk = s // n_chunk
        base = ((1 - chip) * (1 - blk) + chip * blk) * tok_chip
        return pl.multiple_of(base + lax.rem(s, n_chunk) * ROWS, ROWS)

    def finish(s):
        row0 = chunk_row(s)
        rows = pl.ds(row0, ROWS)
        pair_copy(s, row0).wait_recv()
        pbuf[core, rows, :] = pbuf[core, rows, :] + precv[rows, :]

        @pl.when(s < n_chunk)
        def _():
            for p in range(ROWS // PIECE):
                y_copy(s * (ROWS // PIECE) + p).start()

    def chunk(s, carry):
        row0 = chunk_row(s)
        rows = pl.ds(row0, ROWS)
        here = mp[rows, :]
        shift = (me * exp_rows).astype(F32)
        target = here[:, 0:8] + here[:, 16:24] + here[:, 32:40] - shift
        for cb in range(exp_rows // 256):
            col = lax.broadcasted_iota(jnp.int32, (ROWS, 256), 1).astype(F32) + float(cb * 256)
            g0 = jnp.zeros((ROWS, 256), F32)
            g1 = jnp.zeros((ROWS, 256), F32)
            g2 = jnp.zeros((ROWS, 256), F32)
            for j in range(8):
                hit = col == target[:, j:j + 1]
                g0 = jnp.where(hit, here[:, 8 + j:9 + j], g0)
                g1 = jnp.where(hit, here[:, 24 + j:25 + j], g1)
                g2 = jnp.where(hit, here[:, 40 + j:41 + j], g2)
            cols = slice(cb * 256, (cb + 1) * 256)
            gbuf[0:ROWS, cols] = g0.astype(BF16)
            gbuf[ROWS:2 * ROWS, cols] = g1.astype(BF16)
            gbuf[2 * ROWS:3 * ROWS, cols] = g2.astype(BF16)
        lane_h = lax.broadcasted_iota(jnp.int32, (ROWS, LANES), 1).astype(F32)
        is_mine = (tok[rows, :] - (me * tok_dev).astype(F32) == lane_h) & (lane_h < float(tok_dev))
        pick = jnp.where(is_mine, 1.0, 0.0).astype(BF16)[:, :tok_dev]
        for side in range(2):
            hh = (1 - core) if side == 0 else core
            for q in range(4):
                o_cols = wbuf[o_slot + 2 * hh + q // 2, (q % 2) * exp_rows:(q % 2 + 1) * exp_rows, :]
                h_cols = hbuf[:, pl.ds(pl.multiple_of(hh * half + q * gw, gw), gw)]
                p3 = mm(gbuf[...], o_cols)
                total = p3[0:ROWS] + p3[ROWS:2 * ROWS] + p3[2 * ROWS:3 * ROWS] + mm(pick, h_cols)
                pbuf[hh, rows, q * gw:(q + 1) * gw] = total
            if side == 0:
                pair_copy(s, row0).start()

        @pl.when(s > 0)
        def _():
            finish(s - 1)
        return carry

    lax.fori_loop(0, 2 * n_chunk, chunk, 0)
    for t, (g, j) in list(enumerate(first))[o_slot:]:
        qkv_copy(j // 2, j % 2, g, t).start()
    finish(2 * n_chunk - 1)

    def z_copy(k):
        rows = pl.ds(k * PIECE, PIECE)
        return remote(zsend.at[rows], ybuf.at[core, rows], zsnd.at[k], zrcv.at[k], {"pp": nxt})

    def fwd_copy(k):
        rows = pl.ds(k * PIECE, PIECE)
        return remote(ybuf.at[core, rows], ybuf.at[core, rows], fsend.at[k], frcv.at[k], {"ep": partner})

    def norm(k):
        rows = slice(k * PIECE, (k + 1) * PIECE)
        lo = ybuf[0, rows, :].astype(F32)
        hi = ybuf[1, rows, :].astype(F32)
        sq = jnp.sum(lo * lo, axis=-1, keepdims=True) + jnp.sum(hi * hi, axis=-1, keepdims=True)
        inv = lax.rsqrt(sq / float(d_model) + NORM_EPS)
        xbuf[rows, 0:half] = (lo * inv * nw_ref[:, 0:half]).astype(BF16)
        xbuf[rows, half:d_model] = (hi * inv * nw_ref[:, half:d_model]).astype(BF16)

    for k in range(n_piece + 2):
        if k < n_piece:
            y_copy(k).wait_recv()
            near = pl.ds(pl.multiple_of(chip * tok_chip + k * PIECE, PIECE), PIECE)
            rows = slice(k * PIECE, (k + 1) * PIECE)
            zsend[rows, :] = (pbuf[core, near, :] + yrecv[rows, :]).astype(BF16)
            z_copy(k).start()
        if 1 <= k <= n_piece:
            z_copy(k - 1).wait_recv()
            fwd_copy(k - 1).start()
        if k >= 2:
            fwd_copy(k - 2).wait_recv()
            norm(k - 2)

    def a_copy(g):
        return remote(abuf.at[core * n_grp + g], abuf.at[core * n_grp + g], asend.at[g], arcv.at[g], {"ep": partner})

    r_id = lax.broadcasted_iota(jnp.int32, (tok_chip, tok_chip), 0)
    c_id = lax.broadcasted_iota(jnp.int32, (tok_chip, tok_chip), 1)
    mask = (r_id // SEQ == c_id // SEQ) & (c_id <= r_id)

    def group(g, carry):
        base = lax.rem(g, RING_GROUPS) * 6
        for j in range(6):
            qkv_copy(j // 2, j % 2, g, base + j).wait()
        for m in range(3):
            acc = mm(xbuf[:, 0:slot_rows], wbuf[base + 2 * m]) + mm(xbuf[:, slot_rows:2 * slot_rows], wbuf[base + 2 * m + 1])
            qkv[m] = acc.astype(BF16)

        @pl.when(g + RING_GROUPS < n_grp)
        def _():
            for j in range(6):
                qkv_copy(j // 2, j % 2, g + RING_GROUPS, base + j).start()

        for j in range(6):
            w = 6 * (g + RING_GROUPS - n_grp) + j

            @pl.when((w >= 0) & (w < 4 * n_out))
            def _():
                wo_copy(w).start()

        for hd in range(gw // HEAD_DIM):
            cols = slice(hd * HEAD_DIM, (hd + 1) * HEAD_DIM)
            s = mm_t(qkv[0, :, cols], qkv[1, :, cols]) * (HEAD_DIM ** -0.5)
            s = jnp.where(mask, s, -1e30)
            ex = jnp.exp(s - jnp.max(s, axis=-1, keepdims=True))
            prob = (ex / jnp.sum(ex, axis=-1, keepdims=True)).astype(BF16)
            abuf[core * n_grp + g, :, cols] = mm(prob, qkv[2, :, cols]).astype(BF16)
        a_copy(g).start()
        return carry

    lax.fori_loop(0, n_grp, group, 0)

    for g in range(n_grp):
        a_copy(g).wait_recv()

    def out_cols(n):
        return pl.ds(pl.multiple_of(core * half + n * gw, gw), gw)

    def out_local(n):
        rows = pl.ds(pl.multiple_of(core * tok_dev, tok_dev), tok_dev)
        return pltpu.make_async_copy(zbuf.at[n, rows], z_hbm.at[:, out_cols(n)], outl.at[n])

    def out_remote(n):
        rows = pl.ds(pl.multiple_of((1 - core) * tok_dev, tok_dev), tok_dev)
        return remote(zbuf.at[n, rows], z_hbm.at[:, out_cols(n)], outs.at[n], outr.at[n], {"ep": partner})

    def out_group(n, carry):
        for kq in range(4):
            wo_copy(4 * n + kq).wait()
        acc = None
        for kq in range(4):
            slot = lax.rem(6 * n_grp + 4 * n + kq, SLOTS)
            for gg in range(grp_per_slot):
                term = mm(abuf[kq * grp_per_slot + gg], wbuf[slot, gg * gw:(gg + 1) * gw, :])
                acc = term if acc is None else acc + term
        resid = ybuf[core, :, pl.ds(pl.multiple_of(n * gw, gw), gw)].astype(F32)
        zbuf[n] = (resid + acc.astype(BF16).astype(F32)).astype(BF16)
        out_local(n).start()
        out_remote(n).start()
        return carry

    lax.fori_loop(0, n_out, out_group, 0)

    own_copy.wait_send()
    for cp in meta_copies:
        cp.wait_send()
    for s in range(2 * n_chunk):
        pair_copy(s, chunk_row(s)).wait_send()
    for k in range(n_piece):
        y_copy(k).wait_send()
        z_copy(k).wait_send()
        fwd_copy(k).wait_send()
    for g in range(n_grp):
        a_copy(g).wait_send()
    for n in range(n_out):
        out_local(n).wait()
        out_remote(n).wait()


def solution(mesh):
    n_pp = mesh.shape['pp']
    group_axes = ('data', 'pp')

    def device_step(expert_out, expert_id, slot_id, gate, resid, owner, norm_w, w_q, w_k, w_v, w_o):
        d_model = resid.shape[3]
        tok_dev = resid.shape[2]
        n_exp, cap = expert_out.shape[2], expert_out.shape[3]
        exp_rows = n_exp * cap
        width = w_q.shape[2]
        gw = d_model // 8
        n_grp = width // 2 // gw
        n_out = d_model // 2 // gw
        tok_chip = 2 * tok_dev
        half = d_model // 2
        row_id = jnp.where(slot_id[0, 0] >= 0, expert_id[0, 0] * cap + slot_id[0, 0], -1).astype(F32)
        meta = jnp.concatenate([row_id.T, gate[0, 0].T], axis=0)
        meta = jnp.pad(meta, ((0, 0), (0, LANES - tok_dev)))
        own = jnp.broadcast_to(owner[0].astype(F32)[:, None], (owner.shape[1], LANES))
        vmem = pl.BlockSpec(memory_space=pltpu.VMEM)
        anym = pl.BlockSpec(memory_space=pl.ANY)
        dma = pltpu.SemaphoreType.DMA
        n_chunk2 = 2 * tok_chip // ROWS
        n_piece = tok_chip // PIECE
        out = pl.pallas_call(
            functools.partial(stage_kernel, n_pp, gw, exp_rows),
            out_shape=jax.ShapeDtypeStruct((tok_dev, d_model), BF16),
            in_specs=[vmem, vmem, vmem] + [anym] * 6,
            out_specs=anym,
            scratch_shapes=[
                pltpu.VMEM((SLOTS, d_model // 2, gw), BF16),
                pltpu.VMEM((2, 4 * tok_dev, half), F32),
                pltpu.VMEM((4 * tok_dev, half), F32),
                pltpu.VMEM((tok_chip, half), F32),
                pltpu.VMEM((tok_chip, half), BF16),
                pltpu.VMEM((2, tok_chip, half), BF16),
                pltpu.VMEM((tok_chip, d_model), BF16),
                pltpu.VMEM((3, tok_chip, gw), BF16),
                pltpu.VMEM((2 * n_grp, tok_chip, gw), BF16),
                pltpu.VMEM((n_out, tok_chip, gw), BF16),
                pltpu.VMEM((tok_dev, d_model), BF16),
                pltpu.VMEM((3 * ROWS, exp_rows), BF16),
                pltpu.VMEM((N_EP, 16, LANES), F32),
                pltpu.VMEM((4 * SEQ, LANES), F32),
                pltpu.VMEM((4 * tok_dev, LANES), F32),
                pltpu.VMEM((4 * tok_dev, LANES), F32),
                dma((SLOTS,)), dma((8,)), dma,
                dma((3,)), dma((3,)), dma, dma,
                dma((n_chunk2,)), dma((n_chunk2,)),
                dma((n_piece,)), dma((n_piece,)),
                dma((n_piece,)), dma((n_piece,)),
                dma((n_piece,)), dma((n_piece,)),
                dma((n_grp,)), dma((n_grp,)),
                dma((n_out,)), dma((n_out,)), dma((n_out,)),
            ],
            compiler_params=pltpu.CompilerParams(
                collective_id=0, has_side_effects=True, vmem_limit_bytes=67043328),
        )(meta, own, norm_w, expert_out.reshape(exp_rows, d_model), resid.reshape(tok_dev, d_model),
          w_q[0], w_k[0], w_v[0], w_o[0])
        return out.reshape(1, 1, tok_dev, d_model)

    tok_spec = P(group_axes, None, 'ep', None)
    weight_spec = P('pp', None, None)
    in_specs = (P(group_axes, None, 'ep', None, None), tok_spec, tok_spec, tok_spec, tok_spec, P(group_axes, None), P('pp', None), weight_spec, weight_spec, weight_spec, weight_spec)
    return jax.shard_map(device_step, mesh=mesh, in_specs=in_specs, out_specs=tok_spec, check_vma=False)
```

```python
import functools

import jax
import jax.numpy as jnp
from jax import lax
from jax.experimental import pallas as pl
from jax.experimental.pallas import tpu as pltpu
from jax.sharding import PartitionSpec as P

HEAD_DIM = 128
NORM_EPS = 1e-6
SEQ = 8
N_EP = 4
SLOTS = 24
RING_GROUPS = 4
ROWS = 32
PIECE = 16
LANES = 128
BF16_MAX = 3.3895314e38
MESH_ID = pl.DeviceIdType.MESH
F32 = jnp.float32
BF16 = jnp.bfloat16


def mm(a, b):
    return jnp.dot(a, b, preferred_element_type=F32)


def mm_t(a, b):
    return lax.dot_general(a, b, (((1,), (1,)), ((), ())), preferred_element_type=F32)


def split3(x):
    hi = jnp.clip(x, -BF16_MAX, BF16_MAX).astype(BF16)
    r1 = x - hi.astype(F32)
    mid = r1.astype(BF16)
    lo = (r1 - mid.astype(F32)).astype(BF16)
    return hi, mid, lo


def stage_kernel(
    n_pp, gw, exp_rows, cap,
    eid_ref, slot_ref, gate_ref, own_ref, nw_ref, o_hbm, h_hbm, wq_hbm, wk_hbm, wv_hbm, wo_hbm,
    z_hbm,
    wbuf, pbuf, precv, yrecv, zsend, ybuf, xbuf, qkv, abuf, zbuf, hbuf, gbuf, metas, owns, ownr, tok, mp,
    wsem, osem, hsem, msend, mrecv, osend, orecv, psend, prcv, ysend, yrcv, zsnd, zrcv, fsend, frcv, asend, arcv,
    outl, outs, outr,
):
    d_model = nw_ref.shape[1]
    half = d_model // 2
    e_half = wq_hbm.shape[1] // 2
    n_grp = e_half // gw
    slot_rows = wbuf.shape[1]
    n_out = half // gw
    grp_per_slot = slot_rows // gw
    tok_chip = 2 * 8 * SEQ
    tok_dev = 8 * SEQ
    n_chunk = tok_chip // ROWS
    n_piece = tok_chip // PIECE

    me = lax.axis_index("ep")
    core = lax.rem(me, 2)
    chip = me // 2
    partner = chip * 2 + (1 - core)
    across = (1 - chip) * 2 + core
    rank = lax.axis_index("pp")
    nxt = lax.rem(rank + 1, n_pp)
    prv = lax.rem(rank + n_pp - 1, n_pp)

    def remote(src, dst, s_sem, r_sem, dev):
        return pltpu.make_async_remote_copy(
            src_ref=src, dst_ref=dst, send_sem=s_sem, recv_sem=r_sem, device_id=dev, device_id_type=MESH_ID)

    def qkv_copy(mat, kh, g, slot):
        src = (wq_hbm, wk_hbm, wv_hbm)[mat]
        cols = pl.ds(pl.multiple_of(core * e_half + g * gw, gw), gw)
        return pltpu.make_async_copy(
            src.at[pl.ds(pl.multiple_of(kh * slot_rows, slot_rows), slot_rows), cols], wbuf.at[slot], wsem.at[slot])

    def wo_copy(w):
        n, kq = w // 4, lax.rem(w, 4)
        rows = pl.ds(pl.multiple_of(kq * slot_rows, slot_rows), slot_rows)
        cols = pl.ds(pl.multiple_of(core * half + n * gw, gw), gw)
        slot = lax.rem(6 * n_grp + w, SLOTS)
        return pltpu.make_async_copy(wo_hbm.at[rows, cols], wbuf.at[slot], wsem.at[slot])

    o_slot = SLOTS - 4

    def o_copy(nb):
        return pltpu.make_async_copy(
            o_hbm.at[:, pl.ds(nb * gw, gw)],
            wbuf.at[o_slot + nb // 2, pl.ds((nb % 2) * exp_rows, exp_rows)], osem.at[nb])

    h_copy = pltpu.make_async_copy(h_hbm, hbuf, hsem)
    for nb in range(8):
        o_copy(nb).start()
    h_copy.start()

    barrier = pltpu.get_barrier_semaphore()
    for off in (1, 2, 3):
        pl.semaphore_signal(barrier, inc=1, device_id={"ep": lax.rem(me + off, N_EP)}, device_id_type=MESH_ID)
    pl.semaphore_signal(barrier, inc=1, device_id={"pp": nxt}, device_id_type=MESH_ID)
    pl.semaphore_signal(barrier, inc=1, device_id={"pp": prv}, device_id_type=MESH_ID)

    slot = slot_ref[...]
    metas[me] = jnp.zeros((16, LANES), F32)
    metas[me, 0:8, 0:tok_dev] = jnp.where(slot >= 0, eid_ref[...] * cap + slot, -1).astype(F32)
    metas[me, 8:16, 0:tok_dev] = gate_ref[...]
    n_seq = own_ref.shape[1]
    diag = lax.broadcasted_iota(jnp.int32, (n_seq, n_seq), 0) == lax.broadcasted_iota(jnp.int32, (n_seq, n_seq), 1)
    own_row = jnp.broadcast_to(own_ref[...].astype(F32), (n_seq, n_seq))
    own_col = jnp.sum(jnp.where(diag, own_row, 0.0), axis=1, keepdims=True)
    owns[...] = jnp.broadcast_to(own_col, (n_seq, LANES))
    pl.semaphore_wait(barrier, 5)
    own_copy = remote(owns, ownr, osend, orecv, {"pp": prv})
    own_copy.start()
    meta_copies = [
        remote(metas.at[me], metas.at[me], msend.at[off - 1], mrecv.at[off - 1], {"ep": lax.rem(me + off, N_EP)})
        for off in (1, 2, 3)]
    for cp in meta_copies:
        cp.start()
    for step in range(2):
        for m in range(3):
            qkv_copy(m, step, 0, 2 * m + step).start()
    own_copy.wait_recv()
    sub = lax.broadcasted_iota(jnp.int32, (SEQ, LANES), 0).astype(F32)
    for b in range(4 * SEQ):
        row = jnp.broadcast_to(ownr[b:b + 1, :], (SEQ, LANES))
        tok[b * SEQ:(b + 1) * SEQ, :] = row * float(SEQ) + sub
    for cp in meta_copies:
        cp.wait_recv()
    lane = lax.broadcasted_iota(jnp.int32, (4 * tok_dev, LANES), 1).astype(F32)
    routed = None
    for d in range(N_EP):
        hit = (tok[...] - float(d * tok_dev) == lane) & (lane < float(tok_dev))
        perm = jnp.where(hit, 1.0, 0.0).astype(BF16)
        parts = jnp.concatenate(split3(metas[d]), axis=0)
        term = mm_t(perm, parts)
        routed = term if routed is None else routed + term
    mp[:, 0:48] = routed

    for nb in range(8):
        o_copy(nb).wait()
    h_copy.wait()

    def pair_copy(s, row0):
        rows = pl.ds(row0, ROWS)
        return remote(pbuf.at[1 - core, rows], precv.at[rows], psend.at[s], prcv.at[s], {"ep": partner})

    def y_copy(k):
        src = pl.ds(pl.multiple_of((1 - chip) * tok_chip + k * PIECE, PIECE), PIECE)
        dst = pl.ds(pl.multiple_of(k * PIECE, PIECE), PIECE)
        return remote(pbuf.at[core, src], yrecv.at[dst], ysend.at[k], yrcv.at[k], {"ep": across})

    def chunk_row(s):
        blk = s // n_chunk
        base = ((1 - chip) * (1 - blk) + chip * blk) * tok_chip
        return pl.multiple_of(base + lax.rem(s, n_chunk) * ROWS, ROWS)

    def finish(s):
        row0 = chunk_row(s)
        rows = pl.ds(row0, ROWS)
        pair_copy(s, row0).wait_recv()
        pbuf[core, rows, :] = pbuf[core, rows, :] + precv[rows, :]

        @pl.when(s < n_chunk)
        def _():
            for p in range(ROWS // PIECE):
                y_copy(s * (ROWS // PIECE) + p).start()

    def prefetch(t):
        g, kh = t // 2, lax.rem(t, 2)

        @pl.when(t < 2 * RING_GROUPS)
        def _():
            qkv_copy(0, kh, g, 6 * g + kh).start()

        @pl.when(t < 2 * RING_GROUPS - 2)
        def _():
            for m in range(1, 3):
                qkv_copy(m, kh, g, 6 * g + 2 * m + kh).start()

    def chunk(s, carry):
        row0 = chunk_row(s)
        rows = pl.ds(row0, ROWS)
        here = mp[rows, :]
        shift = (me * exp_rows).astype(F32)
        target = here[:, 0:8] + here[:, 16:24] + here[:, 32:40] - shift
        for cb in range(exp_rows // 256):
            col = lax.broadcasted_iota(jnp.int32, (ROWS, 256), 1).astype(F32) + float(cb * 256)
            g0 = jnp.zeros((ROWS, 256), F32)
            g1 = jnp.zeros((ROWS, 256), F32)
            g2 = jnp.zeros((ROWS, 256), F32)
            for j in range(8):
                hit = col == target[:, j:j + 1]
                g0 = jnp.where(hit, here[:, 8 + j:9 + j], g0)
                g1 = jnp.where(hit, here[:, 24 + j:25 + j], g1)
                g2 = jnp.where(hit, here[:, 40 + j:41 + j], g2)
            cols = slice(cb * 256, (cb + 1) * 256)
            gbuf[0:ROWS, cols] = g0.astype(BF16)
            gbuf[ROWS:2 * ROWS, cols] = g1.astype(BF16)
            gbuf[2 * ROWS:3 * ROWS, cols] = g2.astype(BF16)
        lane_h = lax.broadcasted_iota(jnp.int32, (ROWS, LANES), 1).astype(F32)
        is_mine = (tok[rows, :] - (me * tok_dev).astype(F32) == lane_h) & (lane_h < float(tok_dev))
        pick = jnp.where(is_mine, 1.0, 0.0).astype(BF16)[:, :tok_dev]
        for side in range(2):
            hh = (1 - core) if side == 0 else core
            for q in range(4):
                o_cols = wbuf[o_slot + 2 * hh + q // 2, (q % 2) * exp_rows:(q % 2 + 1) * exp_rows, :]
                h_cols = hbuf[:, pl.ds(pl.multiple_of(hh * half + q * gw, gw), gw)]
                p3 = mm(gbuf[...], o_cols)
                total = p3[0:ROWS] + p3[ROWS:2 * ROWS] + p3[2 * ROWS:3 * ROWS] + mm(pick, h_cols)
                pbuf[hh, rows, q * gw:(q + 1) * gw] = total
            if side == 0:
                pair_copy(s, row0).start()
                prefetch(s + 2)

        finish(s)
        return carry

    lax.fori_loop(0, 2 * n_chunk, chunk, 0)
    for kh in range(2):
        for m in range(1, 3):
            qkv_copy(m, kh, RING_GROUPS - 1, SLOTS - 6 + 2 * m + kh).start()

    def z_copy(k):
        rows = pl.ds(k * PIECE, PIECE)
        return remote(zsend.at[rows], ybuf.at[core, rows], zsnd.at[k], zrcv.at[k], {"pp": nxt})

    def fwd_copy(k):
        rows = pl.ds(k * PIECE, PIECE)
        return remote(ybuf.at[core, rows], ybuf.at[core, rows], fsend.at[k], frcv.at[k], {"ep": partner})

    def norm(k):
        rows = slice(k * PIECE, (k + 1) * PIECE)
        lo = ybuf[0, rows, :].astype(F32)
        hi = ybuf[1, rows, :].astype(F32)
        sq = jnp.sum(lo * lo, axis=-1, keepdims=True) + jnp.sum(hi * hi, axis=-1, keepdims=True)
        inv = lax.rsqrt(sq / float(d_model) + NORM_EPS)
        xbuf[rows, 0:half] = (lo * inv * nw_ref[:, 0:half]).astype(BF16)
        xbuf[rows, half:d_model] = (hi * inv * nw_ref[:, half:d_model]).astype(BF16)

    for k in range(n_piece + 2):
        if k < n_piece:
            y_copy(k).wait_recv()
            near = pl.ds(pl.multiple_of(chip * tok_chip + k * PIECE, PIECE), PIECE)
            rows = slice(k * PIECE, (k + 1) * PIECE)
            zsend[rows, :] = (pbuf[core, near, :] + yrecv[rows, :]).astype(BF16)
            z_copy(k).start()
        if 1 <= k <= n_piece:
            z_copy(k - 1).wait_recv()
            fwd_copy(k - 1).start()
        if k >= 2:
            fwd_copy(k - 2).wait_recv()
            norm(k - 2)

    def a_copy(g):
        return remote(abuf.at[core * n_grp + g], abuf.at[core * n_grp + g], asend.at[g], arcv.at[g], {"ep": partner})

    r_id = lax.broadcasted_iota(jnp.int32, (tok_chip, tok_chip), 0)
    c_id = lax.broadcasted_iota(jnp.int32, (tok_chip, tok_chip), 1)
    mask = (r_id // SEQ == c_id // SEQ) & (c_id <= r_id)

    def group(g, carry):
        base = lax.rem(g, RING_GROUPS) * 6
        for j in range(6):
            qkv_copy(j // 2, j % 2, g, base + j).wait()
        for m in range(3):
            acc = mm(xbuf[:, 0:slot_rows], wbuf[base + 2 * m]) + mm(xbuf[:, slot_rows:2 * slot_rows], wbuf[base + 2 * m + 1])
            qkv[m] = acc.astype(BF16)

        @pl.when(g + RING_GROUPS < n_grp)
        def _():
            for j in range(6):
                qkv_copy(j // 2, j % 2, g + RING_GROUPS, base + j).start()

        for j in range(6):
            w = 6 * (g + RING_GROUPS - n_grp) + j

            @pl.when((w >= 0) & (w < 4 * n_out))
            def _():
                wo_copy(w).start()

        for hd in range(gw // HEAD_DIM):
            cols = slice(hd * HEAD_DIM, (hd + 1) * HEAD_DIM)
            s = mm_t(qkv[0, :, cols], qkv[1, :, cols]) * (HEAD_DIM ** -0.5)
            s = jnp.where(mask, s, -1e30)
            ex = jnp.exp(s - jnp.max(s, axis=-1, keepdims=True))
            prob = (ex / jnp.sum(ex, axis=-1, keepdims=True)).astype(BF16)
            abuf[core * n_grp + g, :, cols] = mm(prob, qkv[2, :, cols]).astype(BF16)
        a_copy(g).start()
        return carry

    lax.fori_loop(0, n_grp, group, 0)

    for g in range(n_grp):
        a_copy(g).wait_recv()

    def out_cols(n):
        return pl.ds(pl.multiple_of(core * half + n * gw, gw), gw)

    def out_local(n):
        rows = pl.ds(pl.multiple_of(core * tok_dev, tok_dev), tok_dev)
        return pltpu.make_async_copy(zbuf.at[n, rows], z_hbm.at[:, out_cols(n)], outl.at[n])

    def out_remote(n):
        rows = pl.ds(pl.multiple_of((1 - core) * tok_dev, tok_dev), tok_dev)
        return remote(zbuf.at[n, rows], z_hbm.at[:, out_cols(n)], outs.at[n], outr.at[n], {"ep": partner})

    def out_group(n, carry):
        for kq in range(4):
            wo_copy(4 * n + kq).wait()
        acc = None
        for kq in range(4):
            slot = lax.rem(6 * n_grp + 4 * n + kq, SLOTS)
            for gg in range(grp_per_slot):
                term = mm(abuf[kq * grp_per_slot + gg], wbuf[slot, gg * gw:(gg + 1) * gw, :])
                acc = term if acc is None else acc + term
        resid = ybuf[core, :, pl.ds(pl.multiple_of(n * gw, gw), gw)].astype(F32)
        zbuf[n] = (resid + acc.astype(BF16).astype(F32)).astype(BF16)
        out_local(n).start()
        out_remote(n).start()
        return carry

    lax.fori_loop(0, n_out, out_group, 0)

    own_copy.wait_send()
    for cp in meta_copies:
        cp.wait_send()
    for s in range(2 * n_chunk):
        pair_copy(s, chunk_row(s)).wait_send()
    for k in range(n_piece):
        y_copy(k).wait_send()
        z_copy(k).wait_send()
        fwd_copy(k).wait_send()
    for g in range(n_grp):
        a_copy(g).wait_send()
    for n in range(n_out):
        out_local(n).wait()
        out_remote(n).wait()


def solution(mesh):
    n_pp = mesh.shape['pp']
    group_axes = ('data', 'pp')

    def device_step(expert_out, expert_id, slot_id, gate, resid, owner, norm_w, w_q, w_k, w_v, w_o):
        d_model = resid.shape[3]
        tok_dev = resid.shape[2]
        n_exp, cap = expert_out.shape[2], expert_out.shape[3]
        exp_rows = n_exp * cap
        width = w_q.shape[2]
        gw = d_model // 8
        n_grp = width // 2 // gw
        n_out = d_model // 2 // gw
        tok_chip = 2 * tok_dev
        half = d_model // 2
        vmem = pl.BlockSpec(memory_space=pltpu.VMEM)
        anym = pl.BlockSpec(memory_space=pl.ANY)
        dma = pltpu.SemaphoreType.DMA
        n_chunk2 = 2 * tok_chip // ROWS
        n_piece = tok_chip // PIECE
        out = pl.pallas_call(
            functools.partial(stage_kernel, n_pp, gw, exp_rows, cap),
            out_shape=jax.ShapeDtypeStruct((tok_dev, d_model), BF16),
            in_specs=[vmem] * 5 + [anym] * 6,
            out_specs=anym,
            scratch_shapes=[
                pltpu.VMEM((SLOTS, d_model // 2, gw), BF16),
                pltpu.VMEM((2, 4 * tok_dev, half), F32),
                pltpu.VMEM((4 * tok_dev, half), F32),
                pltpu.VMEM((tok_chip, half), F32),
                pltpu.VMEM((tok_chip, half), BF16),
                pltpu.VMEM((2, tok_chip, half), BF16),
                pltpu.VMEM((tok_chip, d_model), BF16),
                pltpu.VMEM((3, tok_chip, gw), BF16),
                pltpu.VMEM((2 * n_grp, tok_chip, gw), BF16),
                pltpu.VMEM((n_out, tok_chip, gw), BF16),
                pltpu.VMEM((tok_dev, d_model), BF16),
                pltpu.VMEM((3 * ROWS, exp_rows), BF16),
                pltpu.VMEM((N_EP, 16, LANES), F32),
                pltpu.VMEM((4 * SEQ, LANES), F32),
                pltpu.VMEM((4 * SEQ, LANES), F32),
                pltpu.VMEM((4 * tok_dev, LANES), F32),
                pltpu.VMEM((4 * tok_dev, LANES), F32),
                dma((SLOTS,)), dma((8,)), dma,
                dma((3,)), dma((3,)), dma, dma,
                dma((n_chunk2,)), dma((n_chunk2,)),
                dma((n_piece,)), dma((n_piece,)),
                dma((n_piece,)), dma((n_piece,)),
                dma((n_piece,)), dma((n_piece,)),
                dma((n_grp,)), dma((n_grp,)),
                dma((n_out,)), dma((n_out,)), dma((n_out,)),
            ],
            compiler_params=pltpu.CompilerParams(
                collective_id=0, has_side_effects=True, vmem_limit_bytes=67043328),
        )(expert_id[0, 0].T, slot_id[0, 0].T, gate[0, 0].T, owner, norm_w, expert_out.reshape(exp_rows, d_model), resid.reshape(tok_dev, d_model),
          w_q[0], w_k[0], w_v[0], w_o[0])
        return out.reshape(1, 1, tok_dev, d_model)

    tok_spec = P(group_axes, None, 'ep', None)
    weight_spec = P('pp', None, None)
    in_specs = (P(group_axes, None, 'ep', None, None), tok_spec, tok_spec, tok_spec, tok_spec, P(group_axes, None), P('pp', None), weight_spec, weight_spec, weight_spec, weight_spec)
    return jax.shard_map(device_step, mesh=mesh, in_specs=in_specs, out_specs=tok_spec, check_vma=False)
```

```python
import functools

import jax
import jax.numpy as jnp
from jax import lax
from jax.experimental import pallas as pl
from jax.experimental.pallas import tpu as pltpu
from jax.sharding import PartitionSpec as P

HEAD_DIM = 128
NORM_EPS = 1e-6
SEQ = 8
N_EP = 4
SLOTS = 24
RING_GROUPS = 4
ROWS = 32
PIECE = 16
LANES = 128
BF16_MAX = 3.3895314e38
MESH_ID = pl.DeviceIdType.MESH
F32 = jnp.float32
BF16 = jnp.bfloat16


def mm(a, b):
    return jnp.dot(a, b, preferred_element_type=F32)


def mm_t(a, b):
    return lax.dot_general(a, b, (((1,), (1,)), ((), ())), preferred_element_type=F32)


def split3(x):
    hi = jnp.clip(x, -BF16_MAX, BF16_MAX).astype(BF16)
    r1 = x - hi.astype(F32)
    mid = r1.astype(BF16)
    lo = (r1 - mid.astype(F32)).astype(BF16)
    return hi, mid, lo


def stage_kernel(
    n_pp, gw, exp_rows, cap,
    eid_ref, slot_ref, gate_ref, own_ref, nw_ref, o_hbm, h_hbm, wq_hbm, wk_hbm, wv_hbm, wo_hbm,
    z_hbm,
    wbuf, pbuf, precv, yrecv, zsend, ybuf, xbuf, qbuf, kbuf, vbuf, abuf, zbuf, hbuf, gbuf, metas, owns, ownr, tok, mp,
    wsem, osem, hsem, msend, mrecv, osend, orecv, psend, prcv, ysend, yrcv, zsnd, zrcv, fsend, frcv, asend, arcv,
    outl, outs, outr,
):
    d_model = nw_ref.shape[1]
    half = d_model // 2
    e_half = wq_hbm.shape[1] // 2
    n_grp = e_half // gw
    slot_rows = wbuf.shape[1]
    n_out = half // gw
    grp_per_slot = slot_rows // gw
    tok_chip = 2 * 8 * SEQ
    tok_dev = 8 * SEQ
    n_chunk = tok_chip // ROWS
    n_piece = tok_chip // PIECE

    me = lax.axis_index("ep")
    core = lax.rem(me, 2)
    chip = me // 2
    partner = chip * 2 + (1 - core)
    across = (1 - chip) * 2 + core
    rank = lax.axis_index("pp")
    nxt = lax.rem(rank + 1, n_pp)
    prv = lax.rem(rank + n_pp - 1, n_pp)

    def remote(src, dst, s_sem, r_sem, dev):
        return pltpu.make_async_remote_copy(
            src_ref=src, dst_ref=dst, send_sem=s_sem, recv_sem=r_sem, device_id=dev, device_id_type=MESH_ID)

    def qkv_copy(mat, kh, g, slot):
        src = (wq_hbm, wk_hbm, wv_hbm)[mat]
        cols = pl.ds(pl.multiple_of(core * e_half + g * gw, gw), gw)
        return pltpu.make_async_copy(
            src.at[pl.ds(pl.multiple_of(kh * slot_rows, slot_rows), slot_rows), cols], wbuf.at[slot], wsem.at[slot])

    def wo_copy(w):
        n, kq = w // 4, lax.rem(w, 4)
        rows = pl.ds(pl.multiple_of(kq * slot_rows, slot_rows), slot_rows)
        cols = pl.ds(pl.multiple_of(core * half + n * gw, gw), gw)
        slot = lax.rem(6 * n_grp + w, SLOTS)
        return pltpu.make_async_copy(wo_hbm.at[rows, cols], wbuf.at[slot], wsem.at[slot])

    o_slot = SLOTS - 4

    def o_copy(nb):
        return pltpu.make_async_copy(
            o_hbm.at[:, pl.ds(nb * gw, gw)],
            wbuf.at[o_slot + nb // 2, pl.ds((nb % 2) * exp_rows, exp_rows)], osem.at[nb])

    h_copy = pltpu.make_async_copy(h_hbm, hbuf, hsem)
    for nb in range(8):
        o_copy(nb).start()
    h_copy.start()

    barrier = pltpu.get_barrier_semaphore()
    for off in (1, 2, 3):
        pl.semaphore_signal(barrier, inc=1, device_id={"ep": lax.rem(me + off, N_EP)}, device_id_type=MESH_ID)
    pl.semaphore_signal(barrier, inc=1, device_id={"pp": nxt}, device_id_type=MESH_ID)
    pl.semaphore_signal(barrier, inc=1, device_id={"pp": prv}, device_id_type=MESH_ID)

    slot = slot_ref[...]
    metas[me] = jnp.zeros((16, LANES), F32)
    metas[me, 0:8, 0:tok_dev] = jnp.where(slot >= 0, eid_ref[...] * cap + slot, -1).astype(F32)
    metas[me, 8:16, 0:tok_dev] = gate_ref[...]
    n_seq = own_ref.shape[1]
    diag = lax.broadcasted_iota(jnp.int32, (n_seq, n_seq), 0) == lax.broadcasted_iota(jnp.int32, (n_seq, n_seq), 1)
    own_row = jnp.broadcast_to(own_ref[...].astype(F32), (n_seq, n_seq))
    own_col = jnp.sum(jnp.where(diag, own_row, 0.0), axis=1, keepdims=True)
    owns[...] = jnp.broadcast_to(own_col, (n_seq, LANES))
    pl.semaphore_wait(barrier, 5)
    own_copy = remote(owns, ownr, osend, orecv, {"pp": prv})
    own_copy.start()
    meta_copies = [
        remote(metas.at[me], metas.at[me], msend.at[off - 1], mrecv.at[off - 1], {"ep": lax.rem(me + off, N_EP)})
        for off in (1, 2, 3)]
    for cp in meta_copies:
        cp.start()
    for step in range(2):
        for m in range(3):
            qkv_copy(m, step, 0, 2 * m + step).start()
    own_copy.wait_recv()
    sub = lax.broadcasted_iota(jnp.int32, (SEQ, LANES), 0).astype(F32)
    for b in range(4 * SEQ):
        row = jnp.broadcast_to(ownr[b:b + 1, :], (SEQ, LANES))
        tok[b * SEQ:(b + 1) * SEQ, :] = row * float(SEQ) + sub
    for cp in meta_copies:
        cp.wait_recv()
    lane = lax.broadcasted_iota(jnp.int32, (4 * tok_dev, LANES), 1).astype(F32)
    routed = None
    for d in range(N_EP):
        hit = (tok[...] - float(d * tok_dev) == lane) & (lane < float(tok_dev))
        perm = jnp.where(hit, 1.0, 0.0).astype(BF16)
        parts = jnp.concatenate(split3(metas[d]), axis=0)
        term = mm_t(perm, parts)
        routed = term if routed is None else routed + term
    mp[:, 0:48] = routed

    for nb in range(8):
        o_copy(nb).wait()
    h_copy.wait()

    def pair_copy(s, row0):
        rows = pl.ds(row0, ROWS)
        return remote(pbuf.at[1 - core, rows], precv.at[rows], psend.at[s], prcv.at[s], {"ep": partner})

    def y_copy(k):
        src = pl.ds(pl.multiple_of((1 - chip) * tok_chip + k * PIECE, PIECE), PIECE)
        dst = pl.ds(pl.multiple_of(k * PIECE, PIECE), PIECE)
        return remote(pbuf.at[core, src], yrecv.at[dst], ysend.at[k], yrcv.at[k], {"ep": across})

    def chunk_of(s):
        end = 2 * n_chunk - 1
        far = lax.rem(s, 2) + (end - s) // end - s // end
        return far, far * ((s + 1) // 2) + (1 - far) * ((s - 1) // 2)

    def chunk_row(s):
        far, idx = chunk_of(s)
        base = ((1 - chip) * far + chip * (1 - far)) * tok_chip
        return pl.multiple_of(base + idx * ROWS, ROWS)

    def finish(s):
        row0 = chunk_row(s)
        rows = pl.ds(row0, ROWS)
        pair_copy(s, row0).wait_recv()
        pbuf[core, rows, :] = pbuf[core, rows, :] + precv[rows, :]

        far, idx = chunk_of(s)

        @pl.when(far == 1)
        def _():
            for p in range(ROWS // PIECE):
                y_copy(idx * (ROWS // PIECE) + p).start()

    def prefetch(t):
        g, kh = t // 2, lax.rem(t, 2)

        @pl.when(t < 2 * RING_GROUPS)
        def _():
            qkv_copy(0, kh, g, 6 * g + kh).start()

        @pl.when(t < 2 * RING_GROUPS - 2)
        def _():
            for m in range(1, 3):
                qkv_copy(m, kh, g, 6 * g + 2 * m + kh).start()

    def piece(k):
        return pl.ds(pl.multiple_of(k * PIECE, PIECE), PIECE)

    def z_copy(k):
        return remote(zsend.at[piece(k)], ybuf.at[core, piece(k)], zsnd.at[k], zrcv.at[k], {"pp": nxt})

    def fwd_copy(k):
        half_rows = ybuf.at[core, piece(k)]
        return remote(half_rows, half_rows, fsend.at[k], frcv.at[k], {"ep": partner})

    def step_y(k):
        y_copy(k).wait_recv()
        near = pl.ds(pl.multiple_of(chip * tok_chip + k * PIECE, PIECE), PIECE)
        zsend[piece(k), :] = (pbuf[core, near, :] + yrecv[piece(k), :]).astype(BF16)
        z_copy(k).start()

    def step_z(k):
        z_copy(k).wait_recv()
        fwd_copy(k).start()

    def step_norm(k):
        fwd_copy(k).wait_recv()
        rows = piece(k)
        lo = ybuf[0, rows, :].astype(F32)
        hi = ybuf[1, rows, :].astype(F32)
        sq = jnp.sum(lo * lo, axis=-1, keepdims=True) + jnp.sum(hi * hi, axis=-1, keepdims=True)
        inv = lax.rsqrt(sq / float(d_model) + NORM_EPS)
        xbuf[rows, 0:half] = (lo * inv * nw_ref[:, 0:half]).astype(BF16)
        xbuf[rows, half:d_model] = (hi * inv * nw_ref[:, half:d_model]).astype(BF16)

    z_lag, f_lag, first_z = 2, 4, 2

    def chunk(s, carry):
        row0 = chunk_row(s)
        rows = pl.ds(row0, ROWS)
        here = mp[rows, :]
        shift = (me * exp_rows).astype(F32)
        target = here[:, 0:8] + here[:, 16:24] + here[:, 32:40] - shift
        for cb in range(exp_rows // 256):
            col = lax.broadcasted_iota(jnp.int32, (ROWS, 256), 1).astype(F32) + float(cb * 256)
            g0 = jnp.zeros((ROWS, 256), F32)
            g1 = jnp.zeros((ROWS, 256), F32)
            g2 = jnp.zeros((ROWS, 256), F32)
            for j in range(8):
                hit = col == target[:, j:j + 1]
                g0 = jnp.where(hit, here[:, 8 + j:9 + j], g0)
                g1 = jnp.where(hit, here[:, 24 + j:25 + j], g1)
                g2 = jnp.where(hit, here[:, 40 + j:41 + j], g2)
            cols = slice(cb * 256, (cb + 1) * 256)
            gbuf[0:ROWS, cols] = g0.astype(BF16)
            gbuf[ROWS:2 * ROWS, cols] = g1.astype(BF16)
            gbuf[2 * ROWS:3 * ROWS, cols] = g2.astype(BF16)
        lane_h = lax.broadcasted_iota(jnp.int32, (ROWS, LANES), 1).astype(F32)
        is_mine = (tok[rows, :] - (me * tok_dev).astype(F32) == lane_h) & (lane_h < float(tok_dev))
        pick = jnp.where(is_mine, 1.0, 0.0).astype(BF16)[:, :tok_dev]
        for side in range(2):
            hh = (1 - core) if side == 0 else core
            for q in range(4):
                o_cols = wbuf[o_slot + 2 * hh + q // 2, (q % 2) * exp_rows:(q % 2 + 1) * exp_rows, :]
                h_cols = hbuf[:, pl.ds(pl.multiple_of(hh * half + q * gw, gw), gw)]
                p3 = mm(gbuf[...], o_cols)
                total = p3[0:ROWS] + p3[ROWS:2 * ROWS] + p3[2 * ROWS:3 * ROWS] + mm(pick, h_cols)
                pbuf[hh, rows, q * gw:(q + 1) * gw] = total
            if side == 0:
                pair_copy(s, row0).start()
                prefetch(s + 2)

        finish(s)
        for lag, step in ((first_z, step_y), (first_z + z_lag, step_z), (first_z + f_lag, step_norm)):
            @pl.when(s >= lag)
            def _():
                step(s - lag)
        return carry

    lax.fori_loop(0, 2 * n_chunk, chunk, 0)
    for kh in range(2):
        for m in range(1, 3):
            qkv_copy(m, kh, RING_GROUPS - 1, SLOTS - 6 + 2 * m + kh).start()
    for k in range(2 * n_chunk - first_z, n_piece + f_lag):
        if k < n_piece:
            step_y(k)
        if z_lag <= k < n_piece + z_lag:
            step_z(k - z_lag)
        if k >= f_lag:
            step_norm(k - f_lag)

    def a_copy(g):
        return remote(abuf.at[core * n_grp + g], abuf.at[core * n_grp + g], asend.at[g], arcv.at[g], {"ep": partner})

    r_id = lax.broadcasted_iota(jnp.int32, (tok_chip, tok_chip), 0)
    c_id = lax.broadcasted_iota(jnp.int32, (tok_chip, tok_chip), 1)
    mask = (r_id // SEQ == c_id // SEQ) & (c_id <= r_id)

    n_head = gw // HEAD_DIM
    head = [slice(hd * HEAD_DIM, (hd + 1) * HEAD_DIM) for hd in range(n_head)]

    def project(m, base):
        acc = mm(xbuf[:, 0:slot_rows], wbuf[base + 2 * m]) + mm(xbuf[:, slot_rows:2 * slot_rows], wbuf[base + 2 * m + 1])
        return acc.astype(BF16)

    def scores(hd):
        return mm_t(qbuf[:, head[hd]], kbuf[:, head[hd]]) * (HEAD_DIM ** -0.5)

    def softmax(s):
        s = jnp.where(mask, s, -1e30)
        ex = jnp.exp(s - jnp.max(s, axis=-1, keepdims=True))
        return (ex / jnp.sum(ex, axis=-1, keepdims=True)).astype(BF16)

    def mix(g, hd, prob):
        abuf[core * n_grp + g, :, head[hd]] = mm(prob, vbuf[:, head[hd]]).astype(BF16)

    def refill(g, base):
        @pl.when(g + RING_GROUPS < n_grp)
        def _():
            for j in range(6):
                qkv_copy(j // 2, j % 2, g + RING_GROUPS, base + j).start()

        for j in range(6):
            w = 6 * (g + RING_GROUPS - n_grp) + j

            @pl.when((w >= 0) & (w < 4 * n_out))
            def _():
                wo_copy(w).start()

    def wait_group(g, base):
        for j in range(6):
            qkv_copy(j // 2, j % 2, g, base + j).wait()

    wait_group(0, 0)
    qbuf[...] = project(0, 0)
    kbuf[...] = project(1, 0)
    vbuf[...] = project(2, 0)
    refill(0, 0)

    def group(g, carry):
        base = lax.rem(g, RING_GROUPS) * 6
        wait_group(g, base)
        raw = [scores(hd) for hd in range(n_head)]
        q_new = project(0, base)
        probs = [softmax(raw[hd]) for hd in range(n_head)]
        qbuf[...] = q_new
        k_new = project(1, base)
        kbuf[...] = k_new
        for hd in range(n_head):
            mix(g - 1, hd, probs[hd])
        v_new = project(2, base)
        vbuf[...] = v_new
        a_copy(g - 1).start()
        refill(g, base)
        return carry

    lax.fori_loop(1, n_grp, group, 0)
    last = n_grp - 1
    for hd, prob in enumerate([softmax(scores(hd)) for hd in range(n_head)]):
        mix(last, hd, prob)
    a_copy(last).start()

    for g in range(n_grp):
        a_copy(g).wait_recv()

    def out_cols(n):
        return pl.ds(pl.multiple_of(core * half + n * gw, gw), gw)

    def out_local(n):
        rows = pl.ds(pl.multiple_of(core * tok_dev, tok_dev), tok_dev)
        return pltpu.make_async_copy(zbuf.at[n, rows], z_hbm.at[:, out_cols(n)], outl.at[n])

    def out_remote(n):
        rows = pl.ds(pl.multiple_of((1 - core) * tok_dev, tok_dev), tok_dev)
        return remote(zbuf.at[n, rows], z_hbm.at[:, out_cols(n)], outs.at[n], outr.at[n], {"ep": partner})

    def out_group(n, carry):
        for kq in range(4):
            wo_copy(4 * n + kq).wait()
        acc = None
        for kq in range(4):
            slot = lax.rem(6 * n_grp + 4 * n + kq, SLOTS)
            for gg in range(grp_per_slot):
                term = mm(abuf[kq * grp_per_slot + gg], wbuf[slot, gg * gw:(gg + 1) * gw, :])
                acc = term if acc is None else acc + term
        resid = ybuf[core, :, pl.ds(pl.multiple_of(n * gw, gw), gw)].astype(F32)
        zbuf[n] = (resid + acc.astype(BF16).astype(F32)).astype(BF16)
        out_local(n).start()
        out_remote(n).start()
        return carry

    lax.fori_loop(0, n_out, out_group, 0)

    own_copy.wait_send()
    for cp in meta_copies:
        cp.wait_send()
    for s in range(2 * n_chunk):
        pair_copy(s, chunk_row(s)).wait_send()
    for k in range(n_piece):
        y_copy(k).wait_send()
        z_copy(k).wait_send()
        fwd_copy(k).wait_send()
    for g in range(n_grp):
        a_copy(g).wait_send()
    for n in range(n_out):
        out_local(n).wait()
        out_remote(n).wait()


def solution(mesh):
    n_pp = mesh.shape['pp']
    group_axes = ('data', 'pp')

    def device_step(expert_out, expert_id, slot_id, gate, resid, owner, norm_w, w_q, w_k, w_v, w_o):
        d_model = resid.shape[3]
        tok_dev = resid.shape[2]
        n_exp, cap = expert_out.shape[2], expert_out.shape[3]
        exp_rows = n_exp * cap
        width = w_q.shape[2]
        gw = d_model // 8
        n_grp = width // 2 // gw
        n_out = d_model // 2 // gw
        tok_chip = 2 * tok_dev
        half = d_model // 2
        vmem = pl.BlockSpec(memory_space=pltpu.VMEM)
        anym = pl.BlockSpec(memory_space=pl.ANY)
        dma = pltpu.SemaphoreType.DMA
        n_chunk2 = 2 * tok_chip // ROWS
        n_piece = tok_chip // PIECE
        out = pl.pallas_call(
            functools.partial(stage_kernel, n_pp, gw, exp_rows, cap),
            out_shape=jax.ShapeDtypeStruct((tok_dev, d_model), BF16),
            in_specs=[vmem] * 5 + [anym] * 6,
            out_specs=anym,
            scratch_shapes=[
                pltpu.VMEM((SLOTS, d_model // 2, gw), BF16),
                pltpu.VMEM((2, 4 * tok_dev, half), F32),
                pltpu.VMEM((4 * tok_dev, half), F32),
                pltpu.VMEM((tok_chip, half), F32),
                pltpu.VMEM((tok_chip, half), BF16),
                pltpu.VMEM((2, tok_chip, half), BF16),
                pltpu.VMEM((tok_chip, d_model), BF16),
                pltpu.VMEM((tok_chip, gw), BF16),
                pltpu.VMEM((tok_chip, gw), BF16),
                pltpu.VMEM((tok_chip, gw), BF16),
                pltpu.VMEM((2 * n_grp, tok_chip, gw), BF16),
                pltpu.VMEM((n_out, tok_chip, gw), BF16),
                pltpu.VMEM((tok_dev, d_model), BF16),
                pltpu.VMEM((3 * ROWS, exp_rows), BF16),
                pltpu.VMEM((N_EP, 16, LANES), F32),
                pltpu.VMEM((4 * SEQ, LANES), F32),
                pltpu.VMEM((4 * SEQ, LANES), F32),
                pltpu.VMEM((4 * tok_dev, LANES), F32),
                pltpu.VMEM((4 * tok_dev, LANES), F32),
                dma((SLOTS,)), dma((8,)), dma,
                dma((3,)), dma((3,)), dma, dma,
                dma((n_chunk2,)), dma((n_chunk2,)),
                dma((n_piece,)), dma((n_piece,)),
                dma((n_piece,)), dma((n_piece,)),
                dma((n_piece,)), dma((n_piece,)),
                dma((n_grp,)), dma((n_grp,)),
                dma((n_out,)), dma((n_out,)), dma((n_out,)),
            ],
            compiler_params=pltpu.CompilerParams(
                collective_id=0, has_side_effects=True, vmem_limit_bytes=67043328),
        )(expert_id[0, 0].T, slot_id[0, 0].T, gate[0, 0].T, owner, norm_w, expert_out.reshape(exp_rows, d_model), resid.reshape(tok_dev, d_model),
          w_q[0], w_k[0], w_v[0], w_o[0])
        return out.reshape(1, 1, tok_dev, d_model)

    tok_spec = P(group_axes, None, 'ep', None)
    weight_spec = P('pp', None, None)
    in_specs = (P(group_axes, None, 'ep', None, None), tok_spec, tok_spec, tok_spec, tok_spec, P(group_axes, None), P('pp', None), weight_spec, weight_spec, weight_spec, weight_spec)
    return jax.shard_map(device_step, mesh=mesh, in_specs=in_specs, out_specs=tok_spec, check_vma=False)
```

```python
import functools

import jax
import jax.numpy as jnp
from jax import lax
from jax.experimental import pallas as pl
from jax.experimental.pallas import tpu as pltpu
from jax.sharding import PartitionSpec as P

HEAD_DIM = 128
NORM_EPS = 1e-6
SEQ = 8
N_EP = 4
SLOTS = 27
RING_GROUPS = 4
ROWS = 32
PIECE = 16
LANES = 128
BF16_MAX = 3.3895314e38
MESH_ID = pl.DeviceIdType.MESH
F32 = jnp.float32
BF16 = jnp.bfloat16


def mm(a, b):
    return jnp.dot(a, b, preferred_element_type=F32)


def mm_t(a, b):
    return lax.dot_general(a, b, (((1,), (1,)), ((), ())), preferred_element_type=F32)


def split3(x):
    hi = jnp.clip(x, -BF16_MAX, BF16_MAX).astype(BF16)
    r1 = x - hi.astype(F32)
    mid = r1.astype(BF16)
    lo = (r1 - mid.astype(F32)).astype(BF16)
    return hi, mid, lo


def stage_kernel(
    n_pp, gw, exp_rows, cap,
    eid_hbm, slot_hbm, gate_hbm, own_hbm, nw_hbm, o_hbm, h_hbm, wq_hbm, wk_hbm, wv_hbm, wo_hbm,
    z_hbm, y_hbm,
    eid_ref, slot_ref, gate_ref, own_ref, nw_ref, insem, youtsem,
    wbuf, pkeep, pout, precv, yrecv, ybuf, xbuf, qbuf, kbuf, vbuf, abuf, gbuf, metas, owns, ownr, tok, mp,
    wsem, osem, hsem, msend, mrecv, osend, orecv, psend, prcv, ysend, yrcv, zsnd, zrcv, fsend, frcv, asend, arcv,
    outl, outs, outr,
):
    d_model = nw_hbm.shape[1]
    half = d_model // 2
    e_half = wq_hbm.shape[1] // 2
    n_grp = e_half // gw
    slot_rows = wbuf.shape[1]
    n_out = half // gw
    grp_per_slot = slot_rows // gw
    tok_chip = 2 * 8 * SEQ
    tok_dev = 8 * SEQ
    n_chunk = tok_chip // ROWS
    n_piece = tok_chip // PIECE

    me = lax.axis_index("ep")
    core = lax.rem(me, 2)
    chip = me // 2
    partner = chip * 2 + (1 - core)
    across = (1 - chip) * 2 + core
    rank = lax.axis_index("pp")
    nxt = lax.rem(rank + 1, n_pp)
    prv = lax.rem(rank + n_pp - 1, n_pp)

    def remote(src, dst, s_sem, r_sem, dev):
        return pltpu.make_async_remote_copy(
            src_ref=src, dst_ref=dst, send_sem=s_sem, recv_sem=r_sem, device_id=dev, device_id_type=MESH_ID)

    def qkv_copy(mat, kh, g, slot):
        src = (wq_hbm, wk_hbm, wv_hbm)[mat]
        cols = pl.ds(pl.multiple_of(core * e_half + g * gw, gw), gw)
        return pltpu.make_async_copy(
            src.at[pl.ds(pl.multiple_of(kh * slot_rows, slot_rows), slot_rows), cols], wbuf.at[slot], wsem.at[slot])

    def wo_copy(w):
        n, kq = w // 4, lax.rem(w, 4)
        rows = pl.ds(pl.multiple_of(kq * slot_rows, slot_rows), slot_rows)
        cols = pl.ds(pl.multiple_of(core * half + n * gw, gw), gw)
        slot = lax.rem(6 * n_grp + w, SLOTS)
        return pltpu.make_async_copy(wo_hbm.at[rows, cols], wbuf.at[slot], wsem.at[slot])

    o_slot = SLOTS - 4

    def o_copy(nb):
        return pltpu.make_async_copy(
            o_hbm.at[:, pl.ds(nb * gw, gw)],
            wbuf.at[o_slot + nb // 2, pl.ds((nb % 2) * exp_rows, exp_rows)], osem.at[nb])

    def h_copy(nb):
        return pltpu.make_async_copy(
            h_hbm.at[:, pl.ds(nb * gw, gw)], abuf.at[(1 - core) * n_grp + nb, pl.ds(0, tok_dev)], hsem.at[nb])

    barrier = pltpu.get_barrier_semaphore()
    for off in (1, 2, 3):
        pl.semaphore_signal(barrier, inc=1, device_id={"ep": lax.rem(me + off, N_EP)}, device_id_type=MESH_ID)
    pl.semaphore_signal(barrier, inc=1, device_id={"pp": nxt}, device_id_type=MESH_ID)
    pl.semaphore_signal(barrier, inc=1, device_id={"pp": prv}, device_id_type=MESH_ID)
    in_copies = [
        pltpu.make_async_copy(src, dst, insem.at[n]) for n, (src, dst) in enumerate((
            (eid_hbm, eid_ref), (slot_hbm, slot_ref), (gate_hbm, gate_ref), (own_hbm, own_ref), (nw_hbm, nw_ref)))]
    for cp in in_copies:
        cp.start()
    for nb in range(8):
        o_copy(nb).start()
    for nb in range(8):
        h_copy(nb).start()
    for cp in in_copies:
        cp.wait()


    slot = slot_ref[...]
    metas[me] = jnp.zeros((16, LANES), F32)
    metas[me, 0:8, 0:tok_dev] = jnp.where(slot >= 0, eid_ref[...] * cap + slot, -1).astype(F32)
    metas[me, 8:16, 0:tok_dev] = gate_ref[...]
    n_seq = own_ref.shape[1]
    diag = lax.broadcasted_iota(jnp.int32, (n_seq, n_seq), 0) == lax.broadcasted_iota(jnp.int32, (n_seq, n_seq), 1)
    own_row = jnp.broadcast_to(own_ref[...].astype(F32), (n_seq, n_seq))
    own_col = jnp.sum(jnp.where(diag, own_row, 0.0), axis=1, keepdims=True)
    owns[...] = jnp.broadcast_to(own_col, (n_seq, LANES))
    pl.semaphore_wait(barrier, 5)
    own_copy = remote(owns, ownr, osend, orecv, {"pp": prv})
    own_copy.start()
    meta_copies = [
        remote(metas.at[me], metas.at[me], msend.at[off - 1], mrecv.at[off - 1], {"ep": lax.rem(me + off, N_EP)})
        for off in (1, 2, 3)]
    for cp in meta_copies:
        cp.start()
    for step in range(2):
        for m in range(3):
            qkv_copy(m, step, 0, 2 * m + step).start()
    own_copy.wait_recv()
    sub = lax.broadcasted_iota(jnp.int32, (SEQ, LANES), 0).astype(F32)
    for b in range(4 * SEQ):
        row = jnp.broadcast_to(ownr[b:b + 1, :], (SEQ, LANES))
        tok[b * SEQ:(b + 1) * SEQ, :] = row * float(SEQ) + sub
    for cp in meta_copies:
        cp.wait_recv()
    lane = lax.broadcasted_iota(jnp.int32, (4 * tok_dev, LANES), 1).astype(F32)
    routed = None
    for d in range(N_EP):
        hit = (tok[...] - float(d * tok_dev) == lane) & (lane < float(tok_dev))
        perm = jnp.where(hit, 1.0, 0.0).astype(BF16)
        parts = jnp.concatenate(split3(metas[d]), axis=0)
        term = mm_t(perm, parts)
        routed = term if routed is None else routed + term
    mp[:, 0:48] = routed

    for nb in range(8):
        o_copy(nb).wait()
        h_copy(nb).wait()

    def pair_copy(s):
        slot = lax.rem(s, 2)
        return remote(pout.at[slot], precv.at[slot], psend.at[s], prcv.at[s], {"ep": partner})

    def y_copy(k, n):
        src = pl.ds(pl.multiple_of((1 - chip) * tok_chip + k * PIECE, PIECE), n * PIECE)
        dst = pl.ds(pl.multiple_of(k * PIECE, PIECE), n * PIECE)
        return remote(pkeep.at[src], yrecv.at[dst], ysend.at[k], yrcv.at[k], {"ep": across})

    def chunk_of(s):
        end = 2 * n_chunk - 1
        far = lax.rem(s, 2) + (end - s) // end - s // end
        return far, far * ((s + 1) // 2) + (1 - far) * ((s - 1) // 2)

    def chunk_row(s):
        far, idx = chunk_of(s)
        base = ((1 - chip) * far + chip * (1 - far)) * tok_chip
        return pl.multiple_of(base + idx * ROWS, ROWS)

    def finish(s):
        row0 = chunk_row(s)
        rows = pl.ds(row0, ROWS)
        pair_copy(s).wait_recv()
        pkeep[rows, :] = pkeep[rows, :] + precv[lax.rem(s, 2)]

        far, idx = chunk_of(s)

        @pl.when(far * (n_chunk - 1 - idx) > 0)
        def _():
            y_copy(2 * idx, 2).start()

        @pl.when(far * (idx // (n_chunk - 1)) > 0)
        def _():
            y_copy(n_piece - 2, 1).start()
            y_copy(n_piece - 1, 1).start()

    def prefetch(t):
        g, kh = t // 2, lax.rem(t, 2)

        @pl.when(t < 2 * RING_GROUPS)
        def _():
            qkv_copy(0, kh, g, 6 * g + kh).start()
            qkv_copy(1, kh, g, 6 * g + 2 + kh).start()

        @pl.when(t < 2 * RING_GROUPS - 1)
        def _():
            qkv_copy(2, kh, g, 6 * g + 4 + kh).start()

    def piece(k):
        return pl.ds(pl.multiple_of(k * PIECE, PIECE), PIECE)

    def z_copy(k):
        return remote(
            abuf.at[pl.ds(core * n_grp, n_out), piece(k)], ybuf.at[pl.ds(core * n_out, n_out), piece(k)],
            zsnd.at[k], zrcv.at[k], {"pp": nxt})

    def fwd_copy(k):
        half_rows = ybuf.at[pl.ds(core * n_out, n_out), piece(k)]
        return remote(half_rows, half_rows, fsend.at[k], frcv.at[k], {"ep": partner})

    def step_y(k):
        if isinstance(k, int) and k >= n_piece - 2:
            y_copy(k, 1).wait_recv()
        else:
            @pl.when(lax.rem(k, 2) == 0)
            def _():
                y_copy(k, 2).wait_recv()
        near = pl.ds(pl.multiple_of(chip * tok_chip + k * PIECE, PIECE), PIECE)
        for b in range(n_out):
            cols = slice(b * gw, (b + 1) * gw)
            abuf[core * n_grp + b, piece(k), :] = (pkeep[near, cols] + yrecv[piece(k), cols]).astype(BF16)
        z_copy(k).start()

    def step_z(k):
        z_copy(k).wait_recv()
        fwd_copy(k).start()

    def step_norm(k):
        fwd_copy(k).wait_recv()
        rows = piece(k)
        sq = None
        for b in range(2 * n_out):
            val = ybuf[b, rows, :].astype(F32)
            term = jnp.sum(val * val, axis=-1, keepdims=True)
            sq = term if sq is None else sq + term
        inv = lax.rsqrt(sq / float(d_model) + NORM_EPS)
        for b in range(2 * n_out):
            cols = slice(b * gw, (b + 1) * gw)
            xbuf[rows, cols] = (ybuf[b, rows, :].astype(F32) * inv * nw_ref[:, cols]).astype(BF16)

    z_lag, f_lag, first_z = 4, 6, 2

    def chunk(s, carry):
        row0 = chunk_row(s)
        rows = pl.ds(row0, ROWS)
        here = mp[rows, :]
        shift = (me * exp_rows).astype(F32)
        target = here[:, 0:8] + here[:, 16:24] + here[:, 32:40] - shift
        for cb in range(exp_rows // 256):
            col = lax.broadcasted_iota(jnp.int32, (ROWS, 256), 1).astype(F32) + float(cb * 256)
            g0 = jnp.zeros((ROWS, 256), F32)
            g1 = jnp.zeros((ROWS, 256), F32)
            g2 = jnp.zeros((ROWS, 256), F32)
            for j in range(8):
                hit = col == target[:, j:j + 1]
                g0 = jnp.where(hit, here[:, 8 + j:9 + j], g0)
                g1 = jnp.where(hit, here[:, 24 + j:25 + j], g1)
                g2 = jnp.where(hit, here[:, 40 + j:41 + j], g2)
            cols = slice(cb * 256, (cb + 1) * 256)
            gbuf[0:ROWS, cols] = g0.astype(BF16)
            gbuf[ROWS:2 * ROWS, cols] = g1.astype(BF16)
            gbuf[2 * ROWS:3 * ROWS, cols] = g2.astype(BF16)
        lane_h = lax.broadcasted_iota(jnp.int32, (ROWS, LANES), 1).astype(F32)
        is_mine = (tok[rows, :] - (me * tok_dev).astype(F32) == lane_h) & (lane_h < float(tok_dev))
        pick = jnp.where(is_mine, 1.0, 0.0).astype(BF16)[:, :tok_dev]
        @pl.when(s >= 2)
        def _():
            pair_copy(s - 2).wait_send()

        for side in range(2):
            hh = (1 - core) if side == 0 else core
            for q in range(4):
                o_cols = wbuf[o_slot + 2 * hh + q // 2, (q % 2) * exp_rows:(q % 2 + 1) * exp_rows, :]
                h_cols = abuf[(1 - core) * n_grp + hh * n_out + q, 0:tok_dev, :]
                p3 = mm(gbuf[...], o_cols)
                total = p3[0:ROWS] + p3[ROWS:2 * ROWS] + p3[2 * ROWS:3 * ROWS] + mm(pick, h_cols)
                if side == 0:
                    pout[lax.rem(s, 2), :, q * gw:(q + 1) * gw] = total
                else:
                    pkeep[rows, q * gw:(q + 1) * gw] = total
            if side == 0:
                pair_copy(s).start()
                prefetch(s + 2)

        finish(s)
        for lag, step in ((first_z, step_y), (first_z + z_lag, step_z), (first_z + f_lag, step_norm)):
            @pl.when(s >= lag)
            def _():
                step(s - lag)
        return carry

    lax.fori_loop(0, 2 * n_chunk, chunk, 0)
    for t in range(o_slot, SLOTS):
        qkv_copy(t % 6 // 2, t % 2, t // 6, t).start()
    for k in range(2 * n_chunk - first_z, n_piece + f_lag):
        if k < n_piece:
            step_y(k)
        if z_lag <= k < n_piece + z_lag:
            step_z(k - z_lag)
        if k >= f_lag:
            step_norm(k - f_lag)

    def a_copy(g):
        return remote(abuf.at[core * n_grp + g], abuf.at[core * n_grp + g], asend.at[g], arcv.at[g], {"ep": partner})

    r_id = lax.broadcasted_iota(jnp.int32, (tok_chip, tok_chip), 0)
    c_id = lax.broadcasted_iota(jnp.int32, (tok_chip, tok_chip), 1)
    mask = (r_id // SEQ == c_id // SEQ) & (c_id <= r_id)

    n_head = gw // HEAD_DIM
    head = [slice(hd * HEAD_DIM, (hd + 1) * HEAD_DIM) for hd in range(n_head)]

    def slot_of(g, j):
        return lax.rem(6 * g + j, SLOTS)

    def project(m, g):
        acc = mm(xbuf[:, 0:slot_rows], wbuf[slot_of(g, 2 * m)]) + mm(xbuf[:, slot_rows:2 * slot_rows], wbuf[slot_of(g, 2 * m + 1)])
        return acc.astype(BF16)

    def scores(hd):
        return mm_t(qbuf[:, head[hd]], kbuf[:, head[hd]]) * (HEAD_DIM ** -0.5)

    def softmax(s):
        s = jnp.where(mask, s, -1e30)
        ex = jnp.exp(s - jnp.max(s, axis=-1, keepdims=True))
        return (ex / jnp.sum(ex, axis=-1, keepdims=True)).astype(BF16)

    def mix(g, hd, prob):
        abuf[core * n_grp + g, :, head[hd]] = mm(prob, vbuf[:, head[hd]]).astype(BF16)

    def refill(g, j):
        ahead = j + SLOTS
        g2, j2 = g + ahead // 6, ahead % 6

        @pl.when(g2 < n_grp)
        def _():
            qkv_copy(j2 // 2, j2 % 2, g2, slot_of(g, j)).start()

        w = 6 * (g2 - n_grp) + j2

        @pl.when((w >= 0) & (w < 4 * n_out))
        def _():
            wo_copy(w).start()

    def wait_group(g):
        for j in range(6):
            qkv_copy(j // 2, j % 2, g, slot_of(g, j)).wait()

    def y_out(b):
        rows = pl.ds(pl.multiple_of(core * tok_dev, tok_dev), tok_dev)
        return pltpu.make_async_copy(ybuf.at[b, rows], y_hbm.at[:, pl.ds(b * gw, gw)], youtsem.at[b])

    for b in range(2 * n_out):
        y_out(b).start()
    for k in range(n_piece):
        z_copy(k).wait_send()
    wait_group(0)
    for m, buf in enumerate((qbuf, kbuf, vbuf)):
        buf[...] = project(m, 0)
        refill(0, 2 * m)
        refill(0, 2 * m + 1)

    def group(g, carry):
        wait_group(g)
        raw = [scores(hd) for hd in range(n_head)]
        q_new = project(0, g)
        probs = [softmax(raw[hd]) for hd in range(n_head)]
        qbuf[...] = q_new
        k_new = project(1, g)
        kbuf[...] = k_new
        for hd in range(n_head):
            mix(g - 1, hd, probs[hd])
        v_new = project(2, g)
        vbuf[...] = v_new
        a_copy(g - 1).start()
        for j in range(6):
            refill(g, j)
        return carry

    lax.fori_loop(1, n_grp, group, 0)
    last = n_grp - 1
    for hd, prob in enumerate([softmax(scores(hd)) for hd in range(n_head)]):
        mix(last, hd, prob)
    a_copy(last).start()

    for g in range(n_grp):
        a_copy(g).wait_recv()

    def out_cols(n):
        return pl.ds(pl.multiple_of(core * half + n * gw, gw), gw)

    def z_cols(n):
        return pl.ds(pl.multiple_of(n * gw, gw), gw)

    def out_local(n):
        rows = pl.ds(pl.multiple_of(core * tok_dev, tok_dev), tok_dev)
        return pltpu.make_async_copy(xbuf.at[rows, z_cols(n)], z_hbm.at[:, out_cols(n)], outl.at[n])

    def out_remote(n):
        rows = pl.ds(pl.multiple_of((1 - core) * tok_dev, tok_dev), tok_dev)
        return remote(xbuf.at[rows, z_cols(n)], z_hbm.at[:, out_cols(n)], outs.at[n], outr.at[n], {"ep": partner})

    def out_group(n, carry):
        for kq in range(4):
            wo_copy(4 * n + kq).wait()
        acc = None
        for kq in range(4):
            slot = lax.rem(6 * n_grp + 4 * n + kq, SLOTS)
            for gg in range(grp_per_slot):
                term = mm(abuf[kq * grp_per_slot + gg], wbuf[slot, gg * gw:(gg + 1) * gw, :])
                acc = term if acc is None else acc + term
        xbuf[:, z_cols(n)] = acc.astype(BF16)
        out_local(n).start()
        out_remote(n).start()
        return carry

    lax.fori_loop(0, n_out, out_group, 0)

    for b in range(2 * n_out):
        y_out(b).wait()
    own_copy.wait_send()
    for cp in meta_copies:
        cp.wait_send()
    for s in range(2 * n_chunk - 2, 2 * n_chunk):
        pair_copy(s).wait_send()
    for f in range(n_chunk - 1):
        y_copy(2 * f, 2).wait_send()
    for k in (n_piece - 2, n_piece - 1):
        y_copy(k, 1).wait_send()
    for k in range(n_piece):
        fwd_copy(k).wait_send()
    for g in range(n_grp):
        a_copy(g).wait_send()
    for n in range(n_out):
        out_local(n).wait()
        out_remote(n).wait()


def solution(mesh):
    n_pp = mesh.shape['pp']
    group_axes = ('data', 'pp')

    def device_step(expert_out, expert_id, slot_id, gate, resid, owner, norm_w, w_q, w_k, w_v, w_o):
        d_model = resid.shape[3]
        tok_dev = resid.shape[2]
        n_exp, cap = expert_out.shape[2], expert_out.shape[3]
        exp_rows = n_exp * cap
        width = w_q.shape[2]
        gw = d_model // 8
        n_grp = width // 2 // gw
        n_out = d_model // 2 // gw
        tok_chip = 2 * tok_dev
        half = d_model // 2
        anym = pl.BlockSpec(memory_space=pl.ANY)
        dma = pltpu.SemaphoreType.DMA
        n_chunk2 = 2 * tok_chip // ROWS
        n_piece = tok_chip // PIECE
        proj, y_own = pl.pallas_call(
            functools.partial(stage_kernel, n_pp, gw, exp_rows, cap),
            out_shape=[jax.ShapeDtypeStruct((tok_dev, d_model), BF16)] * 2,
            in_specs=[anym] * 11,
            out_specs=[anym] * 2,
            scratch_shapes=[
                pltpu.VMEM((8, tok_dev), jnp.int32),
                pltpu.VMEM((8, tok_dev), jnp.int32),
                pltpu.VMEM((8, tok_dev), F32),
                pltpu.VMEM((1, owner.shape[1]), jnp.int32),
                pltpu.VMEM((1, d_model), F32),
                dma((5,)), dma((8,)),
                pltpu.VMEM((SLOTS, d_model // 2, gw), BF16),
                pltpu.VMEM((4 * tok_dev, half), F32),
                pltpu.VMEM((2, ROWS, half), F32),
                pltpu.VMEM((2, ROWS, half), F32),
                pltpu.VMEM((tok_chip, half), F32),
                pltpu.VMEM((2 * n_out, tok_chip, gw), BF16),
                pltpu.VMEM((tok_chip, d_model), BF16),
                pltpu.VMEM((tok_chip, gw), BF16),
                pltpu.VMEM((tok_chip, gw), BF16),
                pltpu.VMEM((tok_chip, gw), BF16),
                pltpu.VMEM((2 * n_grp, tok_chip, gw), BF16),
                pltpu.VMEM((3 * ROWS, exp_rows), BF16),
                pltpu.VMEM((N_EP, 16, LANES), F32),
                pltpu.VMEM((4 * SEQ, LANES), F32),
                pltpu.VMEM((4 * SEQ, LANES), F32),
                pltpu.VMEM((4 * tok_dev, LANES), F32),
                pltpu.VMEM((4 * tok_dev, LANES), F32),
                dma((SLOTS,)), dma((8,)), dma((8,)),
                dma((3,)), dma((3,)), dma, dma,
                dma((n_chunk2,)), dma((n_chunk2,)),
                dma((n_piece,)), dma((n_piece,)),
                dma((n_piece,)), dma((n_piece,)),
                dma((n_piece,)), dma((n_piece,)),
                dma((n_grp,)), dma((n_grp,)),
                dma((n_out,)), dma((n_out,)), dma((n_out,)),
            ],
            compiler_params=pltpu.CompilerParams(
                collective_id=0, has_side_effects=True, vmem_limit_bytes=67043328),
        )(expert_id[0, 0].T, slot_id[0, 0].T, gate[0, 0].T, owner, norm_w, expert_out.reshape(exp_rows, d_model), resid.reshape(tok_dev, d_model),
          w_q[0], w_k[0], w_v[0], w_o[0])
        out = (y_own.astype(F32) + proj.astype(F32)).astype(BF16)
        return out.reshape(1, 1, tok_dev, d_model)

    tok_spec = P(group_axes, None, 'ep', None)
    weight_spec = P('pp', None, None)
    in_specs = (P(group_axes, None, 'ep', None, None), tok_spec, tok_spec, tok_spec, tok_spec, P(group_axes, None), P('pp', None), weight_spec, weight_spec, weight_spec, weight_spec)
    return jax.shard_map(device_step, mesh=mesh, in_specs=in_specs, out_specs=tok_spec, check_vma=False)
```

```python
import functools

import jax
import jax.numpy as jnp
from jax import lax
from jax.experimental import pallas as pl
from jax.experimental.pallas import tpu as pltpu
from jax.sharding import PartitionSpec as P

HEAD_DIM = 128
NORM_EPS = 1e-6
SEQ = 8
N_EP = 4
SLOTS = 27
RING_GROUPS = 4
ROWS = 32
PIECE = 16
LANES = 128
BF16_MAX = 3.3895314e38
MESH_ID = pl.DeviceIdType.MESH
F32 = jnp.float32
BF16 = jnp.bfloat16


def mm(a, b):
    return jnp.dot(a, b, preferred_element_type=F32)


def mm_t(a, b):
    return lax.dot_general(a, b, (((1,), (1,)), ((), ())), preferred_element_type=F32)


def split3(x):
    hi = jnp.clip(x, -BF16_MAX, BF16_MAX).astype(BF16)
    r1 = x - hi.astype(F32)
    mid = r1.astype(BF16)
    lo = (r1 - mid.astype(F32)).astype(BF16)
    return hi, mid, lo


def stage_kernel(
    n_pp, gw, exp_rows, cap,
    eid_hbm, slot_hbm, gate_hbm, own_hbm, nw_hbm, o_hbm, h_hbm, wq_hbm, wk_hbm, wv_hbm, wo_hbm,
    z_ref,
    eid_ref, slot_ref, gate_ref, own_ref, nw_ref, insem,
    wbuf, pkeep, pout, precv, yrecv, ybuf, xbuf, qbuf, kbuf, vbuf, abuf, metas, owns, tok, mp,
    wsem, osem, hsem, msend, mrecv, osend, orecv, psend, prcv, ysend, yrcv, zsnd, zrcv, fsend, frcv, asend, arcv,
    outs, outr,
):
    d_model = nw_hbm.shape[1]
    half = d_model // 2
    e_half = wq_hbm.shape[1] // 2
    n_grp = e_half // gw
    slot_rows = wbuf.shape[1]
    n_out = half // gw
    grp_per_slot = slot_rows // gw
    tok_chip = 2 * 8 * SEQ
    tok_dev = 8 * SEQ
    n_chunk = tok_chip // ROWS
    n_piece = tok_chip // PIECE

    me = lax.axis_index("ep")
    core = lax.rem(me, 2)
    chip = me // 2
    partner = chip * 2 + (1 - core)
    across = (1 - chip) * 2 + core
    rank = lax.axis_index("pp")
    nxt = lax.rem(rank + 1, n_pp)
    prv = lax.rem(rank + n_pp - 1, n_pp)

    def remote(src, dst, s_sem, r_sem, dev):
        return pltpu.make_async_remote_copy(
            src_ref=src, dst_ref=dst, send_sem=s_sem, recv_sem=r_sem, device_id=dev, device_id_type=MESH_ID)

    def qkv_copy(mat, kh, g, slot):
        src = (wq_hbm, wk_hbm, wv_hbm)[mat]
        cols = pl.ds(pl.multiple_of(core * e_half + g * gw, gw), gw)
        return pltpu.make_async_copy(
            src.at[pl.ds(pl.multiple_of(kh * slot_rows, slot_rows), slot_rows), cols], wbuf.at[slot], wsem.at[slot])

    def wo_copy(w):
        n, kq = w // 4, lax.rem(w, 4)
        rows = pl.ds(pl.multiple_of(kq * slot_rows, slot_rows), slot_rows)
        cols = pl.ds(pl.multiple_of(core * half + n * gw, gw), gw)
        slot = lax.rem(6 * n_grp + w, SLOTS)
        return pltpu.make_async_copy(wo_hbm.at[rows, cols], wbuf.at[slot], wsem.at[slot])

    o_slot = SLOTS - 4

    def o_copy(nb):
        return pltpu.make_async_copy(
            o_hbm.at[:, pl.ds(nb * gw, gw)],
            wbuf.at[o_slot + nb // 2, pl.ds((nb % 2) * exp_rows, exp_rows)], osem.at[nb])

    def h_copy(nb):
        return pltpu.make_async_copy(
            h_hbm.at[:, pl.ds(nb * gw, gw)], abuf.at[(1 - core) * n_grp + nb, pl.ds(0, tok_dev)], hsem.at[nb])

    barrier = pltpu.get_barrier_semaphore()
    for off in (1, 2, 3):
        pl.semaphore_signal(barrier, inc=1, device_id={"ep": lax.rem(me + off, N_EP)}, device_id_type=MESH_ID)
    pl.semaphore_signal(barrier, inc=1, device_id={"pp": nxt}, device_id_type=MESH_ID)
    pl.semaphore_signal(barrier, inc=1, device_id={"pp": prv}, device_id_type=MESH_ID)
    in_copies = [
        pltpu.make_async_copy(src, dst, insem.at[n]) for n, (src, dst) in enumerate((
            (eid_hbm, eid_ref), (slot_hbm, slot_ref), (gate_hbm, gate_ref), (own_hbm, own_ref), (nw_hbm, nw_ref)))]
    for cp in in_copies:
        cp.start()
    for nb in range(8):
        o_copy(nb).start()
    for nb in range(8):
        h_copy(nb).start()
    for cp in in_copies:
        cp.wait()


    slot = slot_ref[...]
    metas[me] = jnp.zeros((16, LANES), F32)
    metas[me, 0:8, 0:tok_dev] = jnp.where(slot >= 0, eid_ref[...] * cap + slot, -1).astype(F32)
    metas[me, 8:16, 0:tok_dev] = gate_ref[...]
    n_seq = own_ref.shape[1]
    diag = lax.broadcasted_iota(jnp.int32, (n_seq, n_seq), 0) == lax.broadcasted_iota(jnp.int32, (n_seq, n_seq), 1)
    own_row = jnp.broadcast_to(own_ref[...].astype(F32), (n_seq, n_seq))
    own_col = jnp.sum(jnp.where(diag, own_row, 0.0), axis=1, keepdims=True)
    owns[...] = jnp.broadcast_to(own_col, (n_seq, LANES))
    pl.semaphore_wait(barrier, 5)
    own_copy = remote(owns, mp.at[pl.ds(0, 4 * SEQ)], osend, orecv, {"pp": prv})
    own_copy.start()
    meta_copies = [
        remote(metas.at[me], metas.at[me], msend.at[off - 1], mrecv.at[off - 1], {"ep": lax.rem(me + off, N_EP)})
        for off in (1, 2, 3)]
    for cp in meta_copies:
        cp.start()
    for step in range(2):
        for m in range(3):
            qkv_copy(m, step, 0, 2 * m + step).start()
    own_copy.wait_recv()
    sub = lax.broadcasted_iota(jnp.int32, (SEQ, LANES), 0).astype(F32)
    for b in range(4 * SEQ):
        row = jnp.broadcast_to(mp[b:b + 1, :], (SEQ, LANES))
        tok[b * SEQ:(b + 1) * SEQ, :] = row * float(SEQ) + sub
    for cp in meta_copies:
        cp.wait_recv()
    lane = lax.broadcasted_iota(jnp.int32, (4 * tok_dev, LANES), 1).astype(F32)
    routed = None
    for d in range(N_EP):
        hit = (tok[...] - float(d * tok_dev) == lane) & (lane < float(tok_dev))
        perm = jnp.where(hit, 1.0, 0.0).astype(BF16)
        parts = jnp.concatenate(split3(metas[d]), axis=0)
        term = mm_t(perm, parts)
        routed = term if routed is None else routed + term
    mp[:, 0:48] = routed

    for nb in range(8):
        o_copy(nb).wait()
        h_copy(nb).wait()

    def pair_copy(s):
        return remote(pout, precv.at[lax.rem(s, 2)], psend.at[s], prcv.at[s], {"ep": partner})

    def y_copy(k, n):
        src = pl.ds(pl.multiple_of((1 - chip) * tok_chip + k * PIECE, PIECE), n * PIECE)
        dst = pl.ds(pl.multiple_of(k * PIECE, PIECE), n * PIECE)
        return remote(pkeep.at[src], yrecv.at[dst], ysend.at[k], yrcv.at[k], {"ep": across})

    def chunk_of(s):
        end = 2 * n_chunk - 1
        far = lax.rem(s, 2) + (end - s) // end - s // end
        return far, far * ((s + 1) // 2) + (1 - far) * ((s - 1) // 2)

    def chunk_row(s):
        far, idx = chunk_of(s)
        base = ((1 - chip) * far + chip * (1 - far)) * tok_chip
        return pl.multiple_of(base + idx * ROWS, ROWS)

    def finish(s):
        row0 = chunk_row(s)
        rows = pl.ds(row0, ROWS)
        pair_copy(s).wait_recv()
        pkeep[rows, :] = pkeep[rows, :] + precv[lax.rem(s, 2)]

        far, idx = chunk_of(s)

        @pl.when(far * (n_chunk - 1 - idx) > 0)
        def _():
            y_copy(2 * idx, 2).start()

        @pl.when(far * (idx // (n_chunk - 1)) > 0)
        def _():
            y_copy(n_piece - 2, 1).start()
            y_copy(n_piece - 1, 1).start()

    def prefetch(t):
        g, kh = t // 2, lax.rem(t, 2)

        @pl.when(t < 2 * RING_GROUPS)
        def _():
            qkv_copy(0, kh, g, 6 * g + kh).start()
            qkv_copy(1, kh, g, 6 * g + 2 + kh).start()

        @pl.when(t < 2 * RING_GROUPS - 1)
        def _():
            qkv_copy(2, kh, g, 6 * g + 4 + kh).start()

    def piece(k):
        return pl.ds(pl.multiple_of(k * PIECE, PIECE), PIECE)

    def z_copy(k):
        return remote(
            abuf.at[pl.ds(core * n_grp, n_out), piece(k)], ybuf.at[pl.ds(core * n_out, n_out), piece(k)],
            zsnd.at[k], zrcv.at[k], {"pp": nxt})

    def fwd_copy(k):
        half_rows = ybuf.at[pl.ds(core * n_out, n_out), piece(k)]
        return remote(half_rows, half_rows, fsend.at[k], frcv.at[k], {"ep": partner})

    def step_y(k):
        if isinstance(k, int) and k >= n_piece - 2:
            y_copy(k, 1).wait_recv()
        else:
            @pl.when(lax.rem(k, 2) == 0)
            def _():
                y_copy(k, 2).wait_recv()
        near = pl.ds(pl.multiple_of(chip * tok_chip + k * PIECE, PIECE), PIECE)
        for b in range(n_out):
            cols = slice(b * gw, (b + 1) * gw)
            abuf[core * n_grp + b, piece(k), :] = (pkeep[near, cols] + yrecv[piece(k), cols]).astype(BF16)
        z_copy(k).start()

    def step_z(k):
        z_copy(k).wait_recv()
        fwd_copy(k).start()

    def step_norm(k):
        fwd_copy(k).wait_recv()
        rows = piece(k)
        sq = None
        for b in range(2 * n_out):
            val = ybuf[b, rows, :].astype(F32)
            term = jnp.sum(val * val, axis=-1, keepdims=True)
            sq = term if sq is None else sq + term
        inv = lax.rsqrt(sq / float(d_model) + NORM_EPS)
        for b in range(2 * n_out):
            cols = slice(b * gw, (b + 1) * gw)
            xbuf[rows, cols] = (ybuf[b, rows, :].astype(F32) * inv * nw_ref[:, cols]).astype(BF16)

    z_lag, f_lag, first_z = 4, 6, 2

    g_blk = core * n_grp + n_out
    gcol = min(256, gw)

    def chunk(s, carry):
        row0 = chunk_row(s)
        rows = pl.ds(row0, ROWS)
        here = mp[rows, :]
        shift = (me * exp_rows).astype(F32)
        target = here[:, 0:8] + here[:, 16:24] + here[:, 32:40] - shift
        for cb in range(exp_rows // 256):
            col = lax.broadcasted_iota(jnp.int32, (ROWS, 256), 1).astype(F32) + float(cb * 256)
            g0 = jnp.zeros((ROWS, 256), F32)
            g1 = jnp.zeros((ROWS, 256), F32)
            g2 = jnp.zeros((ROWS, 256), F32)
            for j in range(8):
                hit = col == target[:, j:j + 1]
                g0 = jnp.where(hit, here[:, 8 + j:9 + j], g0)
                g1 = jnp.where(hit, here[:, 24 + j:25 + j], g1)
                g2 = jnp.where(hit, here[:, 40 + j:41 + j], g2)
            for part, val in enumerate((g0, g1, g2)):
                for c0 in range(0, 256, gcol):
                    at = cb * 256 + c0
                    abuf[g_blk + at // gw, part * ROWS:(part + 1) * ROWS, at % gw:at % gw + gcol] = val[:, c0:c0 + gcol].astype(BF16)
        lane_h = lax.broadcasted_iota(jnp.int32, (ROWS, LANES), 1).astype(F32)
        is_mine = (tok[rows, :] - (me * tok_dev).astype(F32) == lane_h) & (lane_h < float(tok_dev))
        pick = jnp.where(is_mine, 1.0, 0.0).astype(BF16)[:, :tok_dev]
        @pl.when(s >= 1)
        def _():
            pair_copy(s - 1).wait_send()

        for side in range(2):
            hh = (1 - core) if side == 0 else core
            for q in range(4):
                o_cols = wbuf[o_slot + 2 * hh + q // 2, (q % 2) * exp_rows:(q % 2 + 1) * exp_rows, :]
                h_cols = abuf[(1 - core) * n_grp + hh * n_out + q, 0:tok_dev, :]
                p3 = None
                for kb in range(exp_rows // gw):
                    term = mm(abuf[g_blk + kb, 0:3 * ROWS, :], o_cols[kb * gw:(kb + 1) * gw, :])
                    p3 = term if p3 is None else p3 + term
                total = p3[0:ROWS] + p3[ROWS:2 * ROWS] + p3[2 * ROWS:3 * ROWS] + mm(pick, h_cols)
                if side == 0:
                    pout[:, q * gw:(q + 1) * gw] = total
                else:
                    pkeep[rows, q * gw:(q + 1) * gw] = total
            if side == 0:
                pair_copy(s).start()
                prefetch(s + 2)

        finish(s)
        for lag, step in ((first_z, step_y), (first_z + z_lag, step_z), (first_z + f_lag, step_norm)):
            @pl.when(s >= lag)
            def _():
                step(s - lag)
        return carry

    lax.fori_loop(0, 2 * n_chunk, chunk, 0)
    for t in range(o_slot, SLOTS):
        qkv_copy(t % 6 // 2, t % 2, t // 6, t).start()
    for k in range(2 * n_chunk - first_z, n_piece + f_lag):
        if k < n_piece:
            step_y(k)
        if z_lag <= k < n_piece + z_lag:
            step_z(k - z_lag)
        if k >= f_lag:
            step_norm(k - f_lag)

    def a_copy(g):
        return remote(abuf.at[core * n_grp + g], abuf.at[core * n_grp + g], asend.at[g], arcv.at[g], {"ep": partner})

    r_id = lax.broadcasted_iota(jnp.int32, (tok_chip, tok_chip), 0)
    c_id = lax.broadcasted_iota(jnp.int32, (tok_chip, tok_chip), 1)
    mask = (r_id // SEQ == c_id // SEQ) & (c_id <= r_id)

    n_head = gw // HEAD_DIM
    head = [slice(hd * HEAD_DIM, (hd + 1) * HEAD_DIM) for hd in range(n_head)]

    def slot_of(g, j):
        return lax.rem(6 * g + j, SLOTS)

    def project(m, g):
        acc = mm(xbuf[:, 0:slot_rows], wbuf[slot_of(g, 2 * m)]) + mm(xbuf[:, slot_rows:2 * slot_rows], wbuf[slot_of(g, 2 * m + 1)])
        return acc.astype(BF16)

    def scores(hd):
        return mm_t(qbuf[:, head[hd]], kbuf[:, head[hd]]) * (HEAD_DIM ** -0.5)

    def softmax(s):
        s = jnp.where(mask, s, -1e30)
        ex = jnp.exp(s - jnp.max(s, axis=-1, keepdims=True))
        return (ex / jnp.sum(ex, axis=-1, keepdims=True)).astype(BF16)

    def mix(g, hd, prob):
        abuf[core * n_grp + g, :, head[hd]] = mm(prob, vbuf[:, head[hd]]).astype(BF16)

    def refill(g, j):
        ahead = j + SLOTS
        g2, j2 = g + ahead // 6, ahead % 6

        @pl.when(g2 < n_grp)
        def _():
            qkv_copy(j2 // 2, j2 % 2, g2, slot_of(g, j)).start()

        w = 6 * (g2 - n_grp) + j2

        @pl.when((w >= 0) & (w < 4 * n_out))
        def _():
            wo_copy(w).start()

    def wait_group(g):
        for j in range(6):
            qkv_copy(j // 2, j % 2, g, slot_of(g, j)).wait()

    for k in range(n_piece):
        z_copy(k).wait_send()
    wait_group(0)
    for m, buf in enumerate((qbuf, kbuf, vbuf)):
        buf[...] = project(m, 0)
        refill(0, 2 * m)
        refill(0, 2 * m + 1)

    def group(g, carry):
        wait_group(g)
        raw = [scores(hd) for hd in range(n_head)]
        q_new = project(0, g)
        probs = [softmax(raw[hd]) for hd in range(n_head)]
        qbuf[...] = q_new
        k_new = project(1, g)
        kbuf[...] = k_new
        for hd in range(n_head):
            mix(g - 1, hd, probs[hd])
        v_new = project(2, g)
        vbuf[...] = v_new
        a_copy(g - 1).start()
        for j in range(6):
            refill(g, j)
        return carry

    lax.fori_loop(1, n_grp, group, 0)
    last = n_grp - 1
    for hd, prob in enumerate([softmax(scores(hd)) for hd in range(n_head)]):
        mix(last, hd, prob)
    a_copy(last).start()

    for g in range(n_grp):
        a_copy(g).wait_recv()

    def out_cols(n):
        return pl.ds(pl.multiple_of(core * half + n * gw, gw), gw)

    def z_cols(n):
        return pl.ds(pl.multiple_of(n * gw, gw), gw)

    def out_remote(n):
        rows = pl.ds(pl.multiple_of((1 - core) * tok_dev, tok_dev), tok_dev)
        return remote(xbuf.at[rows, z_cols(n)], z_ref.at[:, out_cols(n)], outs.at[n], outr.at[n], {"ep": partner})

    def out_part(n, kq):
        slot = lax.rem(6 * n_grp + 4 * n + kq, SLOTS)
        acc = None
        for gg in range(grp_per_slot):
            term = mm(abuf[kq * grp_per_slot + gg], wbuf[slot, gg * gw:(gg + 1) * gw, :])
            acc = term if acc is None else acc + term
        return acc

    def out_done(n, acc):
        resid = ybuf[core * n_out + n].astype(F32)
        xbuf[:, z_cols(n)] = (resid + acc.astype(BF16).astype(F32)).astype(BF16)
        out_remote(n).start()
        mine = pl.ds(pl.multiple_of(core * tok_dev, tok_dev), tok_dev)
        z_ref[:, out_cols(n)] = xbuf[mine, z_cols(n)]

    def out_group(n, carry):
        for kq in range(4):
            wo_copy(4 * n + kq).wait()
        out_done(n, out_part(n, 0) + out_part(n, 1) + out_part(n, 2) + out_part(n, 3))
        return carry

    lax.fori_loop(0, n_out - 1, out_group, 0)
    end = n_out - 1
    total = None
    for kq in range(4):
        wo_copy(4 * end + kq).wait()
        part = out_part(end, kq)
        total = part if total is None else total + part
    out_done(end, total)

    own_copy.wait_send()
    for cp in meta_copies:
        cp.wait_send()
    pair_copy(2 * n_chunk - 1).wait_send()
    for f in range(n_chunk - 1):
        y_copy(2 * f, 2).wait_send()
    for k in (n_piece - 2, n_piece - 1):
        y_copy(k, 1).wait_send()
    for k in range(n_piece):
        fwd_copy(k).wait_send()
    for g in range(n_grp):
        a_copy(g).wait_send()
    for n in range(n_out):
        out_remote(n).wait()


def solution(mesh):
    n_pp = mesh.shape['pp']
    group_axes = ('data', 'pp')

    def device_step(expert_out, expert_id, slot_id, gate, resid, owner, norm_w, w_q, w_k, w_v, w_o):
        d_model = resid.shape[3]
        tok_dev = resid.shape[2]
        n_exp, cap = expert_out.shape[2], expert_out.shape[3]
        exp_rows = n_exp * cap
        width = w_q.shape[2]
        gw = d_model // 8
        n_grp = width // 2 // gw
        n_out = d_model // 2 // gw
        tok_chip = 2 * tok_dev
        half = d_model // 2
        anym = pl.BlockSpec(memory_space=pl.ANY)
        dma = pltpu.SemaphoreType.DMA
        n_chunk2 = 2 * tok_chip // ROWS
        n_piece = tok_chip // PIECE
        out = pl.pallas_call(
            functools.partial(stage_kernel, n_pp, gw, exp_rows, cap),
            out_shape=pltpu.VMEM((tok_dev, d_model), BF16),
            in_specs=[anym] * 11,
            out_specs=pl.BlockSpec(memory_space=pltpu.VMEM),
            scratch_shapes=[
                pltpu.VMEM((8, tok_dev), jnp.int32),
                pltpu.VMEM((8, tok_dev), jnp.int32),
                pltpu.VMEM((8, tok_dev), F32),
                pltpu.VMEM((1, owner.shape[1]), jnp.int32),
                pltpu.VMEM((1, d_model), F32),
                dma((5,)),
                pltpu.VMEM((SLOTS, d_model // 2, gw), BF16),
                pltpu.VMEM((4 * tok_dev, half), F32),
                pltpu.VMEM((ROWS, half), F32),
                pltpu.VMEM((2, ROWS, half), F32),
                pltpu.VMEM((tok_chip, half), F32),
                pltpu.VMEM((2 * n_out, tok_chip, gw), BF16),
                pltpu.VMEM((tok_chip, d_model), BF16),
                pltpu.VMEM((tok_chip, gw), BF16),
                pltpu.VMEM((tok_chip, gw), BF16),
                pltpu.VMEM((tok_chip, gw), BF16),
                pltpu.VMEM((2 * n_grp, tok_chip, gw), BF16),
                pltpu.VMEM((N_EP, 16, LANES), F32),
                pltpu.VMEM((4 * SEQ, LANES), F32),
                pltpu.VMEM((4 * tok_dev, LANES), F32),
                pltpu.VMEM((4 * tok_dev, LANES), F32),
                dma((SLOTS,)), dma((8,)), dma((8,)),
                dma((3,)), dma((3,)), dma, dma,
                dma((n_chunk2,)), dma((n_chunk2,)),
                dma((n_piece,)), dma((n_piece,)),
                dma((n_piece,)), dma((n_piece,)),
                dma((n_piece,)), dma((n_piece,)),
                dma((n_grp,)), dma((n_grp,)),
                dma((n_out,)), dma((n_out,)),
            ],
            compiler_params=pltpu.CompilerParams(
                collective_id=0, has_side_effects=True, vmem_limit_bytes=66519040),
        )(expert_id[0, 0].T, slot_id[0, 0].T, gate[0, 0].T, owner, norm_w, expert_out.reshape(exp_rows, d_model), resid.reshape(tok_dev, d_model),
          w_q[0], w_k[0], w_v[0], w_o[0])
        return out.reshape(1, 1, tok_dev, d_model)

    tok_spec = P(group_axes, None, 'ep', None)
    weight_spec = P('pp', None, None)
    in_specs = (P(group_axes, None, 'ep', None, None), tok_spec, tok_spec, tok_spec, tok_spec, P(group_axes, None), P('pp', None), weight_spec, weight_spec, weight_spec, weight_spec)
    return jax.shard_map(device_step, mesh=mesh, in_specs=in_specs, out_specs=tok_spec, check_vma=False)
```

```python
import functools

import jax
import jax.numpy as jnp
from jax import lax
from jax.experimental import pallas as pl
from jax.experimental.pallas import tpu as pltpu
from jax.sharding import PartitionSpec as P

HEAD_DIM = 128
NORM_EPS = 1e-6
SEQ = 8
N_EP = 4
SLOTS = 27
RING_GROUPS = 4
ROWS = 32
PIECE = 16
LANES = 128
BF16_MAX = 3.3895314e38
MESH_ID = pl.DeviceIdType.MESH
F32 = jnp.float32
BF16 = jnp.bfloat16


def mm(a, b):
    return jnp.dot(a, b, preferred_element_type=F32)


def mm_t(a, b):
    return lax.dot_general(a, b, (((1,), (1,)), ((), ())), preferred_element_type=F32)


def split3(x):
    hi = jnp.clip(x, -BF16_MAX, BF16_MAX).astype(BF16)
    r1 = x - hi.astype(F32)
    mid = r1.astype(BF16)
    lo = (r1 - mid.astype(F32)).astype(BF16)
    return hi, mid, lo


def stage_kernel(
    n_pp, gw, exp_rows, cap,
    eid_hbm, slot_hbm, gate_hbm, own_hbm, nw_hbm, o_hbm, h_hbm, wq_hbm, wk_hbm, wv_hbm, wo_hbm,
    z_ref,
    eid_ref, slot_ref, gate_ref, own_ref, nw_ref, insem,
    wbuf, pkeep, pout, precv, yrecv, ybuf, xbuf, qbuf, kbuf, vbuf, abuf, metas, owns, tok, mp,
    wsem, osem, hsem, msend, mrecv, osend, orecv, psend, prcv, ysend, yrcv, zsnd, zrcv, fsend, frcv, asend, arcv,
    outs, outr,
):
    d_model = nw_hbm.shape[1]
    half = d_model // 2
    e_half = wq_hbm.shape[1] // 2
    n_grp = e_half // gw
    slot_rows = wbuf.shape[1]
    n_out = half // gw
    grp_per_slot = slot_rows // gw
    tok_chip = 2 * 8 * SEQ
    tok_dev = 8 * SEQ
    n_chunk = tok_chip // ROWS
    n_piece = tok_chip // PIECE

    me = lax.axis_index("ep")
    core = lax.rem(me, 2)
    chip = me // 2
    partner = chip * 2 + (1 - core)
    across = (1 - chip) * 2 + core
    rank = lax.axis_index("pp")
    nxt = lax.rem(rank + 1, n_pp)
    prv = lax.rem(rank + n_pp - 1, n_pp)

    def remote(src, dst, s_sem, r_sem, dev):
        return pltpu.make_async_remote_copy(
            src_ref=src, dst_ref=dst, send_sem=s_sem, recv_sem=r_sem, device_id=dev, device_id_type=MESH_ID)

    def qkv_copy(mat, kh, g, slot):
        src = (wq_hbm, wk_hbm, wv_hbm)[mat]
        cols = pl.ds(pl.multiple_of(core * e_half + g * gw, gw), gw)
        return pltpu.make_async_copy(
            src.at[pl.ds(pl.multiple_of(kh * slot_rows, slot_rows), slot_rows), cols], wbuf.at[slot], wsem.at[slot])

    def wo_copy(w):
        n, kq = w // 4, lax.rem(w, 4)
        rows = pl.ds(pl.multiple_of(kq * slot_rows, slot_rows), slot_rows)
        cols = pl.ds(pl.multiple_of(core * half + n * gw, gw), gw)
        slot = lax.rem(6 * n_grp + w, SLOTS)
        return pltpu.make_async_copy(wo_hbm.at[rows, cols], wbuf.at[slot], wsem.at[slot])

    o_slot = SLOTS - 4

    def o_copy(nb):
        return pltpu.make_async_copy(
            o_hbm.at[:, pl.ds(nb * gw, gw)],
            wbuf.at[o_slot + nb // 2, pl.ds((nb % 2) * exp_rows, exp_rows)], osem.at[nb])

    def h_copy(nb):
        return pltpu.make_async_copy(
            h_hbm.at[:, pl.ds(nb * gw, gw)], abuf.at[(1 - core) * n_grp + nb, pl.ds(0, tok_dev)], hsem.at[nb])

    barrier = pltpu.get_barrier_semaphore()
    for off in (1, 2, 3):
        pl.semaphore_signal(barrier, inc=1, device_id={"ep": lax.rem(me + off, N_EP)}, device_id_type=MESH_ID)
    pl.semaphore_signal(barrier, inc=1, device_id={"pp": nxt}, device_id_type=MESH_ID)
    pl.semaphore_signal(barrier, inc=1, device_id={"pp": prv}, device_id_type=MESH_ID)
    in_copies = [
        pltpu.make_async_copy(src, dst, insem.at[n]) for n, (src, dst) in enumerate((
            (eid_hbm, eid_ref), (slot_hbm, slot_ref), (gate_hbm, gate_ref), (own_hbm, own_ref), (nw_hbm, nw_ref)))]
    for cp in in_copies:
        cp.start()
    for nb in range(8):
        o_copy(nb).start()
    for nb in range(8):
        h_copy(nb).start()
    for cp in in_copies:
        cp.wait()


    slot = slot_ref[...]
    metas[me] = jnp.zeros((16, LANES), F32)
    metas[me, 0:8, 0:tok_dev] = jnp.where(slot >= 0, eid_ref[...] * cap + slot, -1).astype(F32)
    metas[me, 8:16, 0:tok_dev] = gate_ref[...]
    n_seq = own_ref.shape[1]
    diag = lax.broadcasted_iota(jnp.int32, (n_seq, n_seq), 0) == lax.broadcasted_iota(jnp.int32, (n_seq, n_seq), 1)
    own_row = jnp.broadcast_to(own_ref[...].astype(F32), (n_seq, n_seq))
    own_col = jnp.sum(jnp.where(diag, own_row, 0.0), axis=1, keepdims=True)
    owns[...] = jnp.broadcast_to(own_col, (n_seq, LANES))
    pl.semaphore_wait(barrier, 5)
    own_copy = remote(owns, mp.at[pl.ds(0, 4 * SEQ)], osend, orecv, {"pp": prv})
    own_copy.start()
    meta_copies = [
        remote(metas.at[me], metas.at[me], msend.at[off - 1], mrecv.at[off - 1], {"ep": lax.rem(me + off, N_EP)})
        for off in (1, 2, 3)]
    for cp in meta_copies:
        cp.start()
    for step in range(2):
        for m in range(3):
            qkv_copy(m, step, 0, 2 * m + step).start()
    own_copy.wait_recv()
    sub = lax.broadcasted_iota(jnp.int32, (SEQ, LANES), 0).astype(F32)
    for b in range(4 * SEQ):
        row = jnp.broadcast_to(mp[b:b + 1, :], (SEQ, LANES))
        tok[b * SEQ:(b + 1) * SEQ, :] = row * float(SEQ) + sub
    for cp in meta_copies:
        cp.wait_recv()
    lane = lax.broadcasted_iota(jnp.int32, (4 * tok_dev, LANES), 1).astype(F32)
    routed = None
    for d in range(N_EP):
        hit = (tok[...] - float(d * tok_dev) == lane) & (lane < float(tok_dev))
        perm = jnp.where(hit, 1.0, 0.0).astype(BF16)
        parts = jnp.concatenate(split3(metas[d]), axis=0)
        term = mm_t(perm, parts)
        routed = term if routed is None else routed + term
    mp[:, 0:48] = routed

    for nb in range(8):
        o_copy(nb).wait()
        h_copy(nb).wait()

    def pair_copy(s):
        return remote(pout, precv.at[lax.rem(s, 2)], psend.at[s], prcv.at[s], {"ep": partner})

    def y_copy(k, n):
        src = pl.ds(pl.multiple_of((1 - chip) * tok_chip + k * PIECE, PIECE), n * PIECE)
        dst = pl.ds(pl.multiple_of(k * PIECE, PIECE), n * PIECE)
        return remote(pkeep.at[src], yrecv.at[dst], ysend.at[k], yrcv.at[k], {"ep": across})

    def y_tail(h):
        src = pl.ds(pl.multiple_of((1 - chip) * tok_chip + (n_piece - 1) * PIECE, PIECE), PIECE)
        dst = pl.ds((n_piece - 1) * PIECE, PIECE)
        cols = pl.ds(h * (half // 2), half // 2)
        at = n_piece - 1 + h
        return remote(pkeep.at[src, cols], yrecv.at[dst, cols], ysend.at[at], yrcv.at[at], {"ep": across})

    def chunk_of(s):
        end = 2 * n_chunk - 1
        far = lax.rem(s, 2) + (end - s) // end - s // end
        return far, far * ((s + 1) // 2) + (1 - far) * ((s - 1) // 2)

    def chunk_row(s):
        far, idx = chunk_of(s)
        base = ((1 - chip) * far + chip * (1 - far)) * tok_chip
        return pl.multiple_of(base + idx * ROWS, ROWS)

    def finish(s):
        row0 = chunk_row(s)
        rows = pl.ds(row0, ROWS)
        pair_copy(s).wait_recv()
        pkeep[rows, :] = pkeep[rows, :] + precv[lax.rem(s, 2)]

        far, idx = chunk_of(s)

        @pl.when(far * (n_chunk - 1 - idx) > 0)
        def _():
            y_copy(2 * idx, 2).start()

        @pl.when(far * (idx // (n_chunk - 1)) > 0)
        def _():
            y_copy(n_piece - 2, 1).start()
            y_tail(0).start()
            y_tail(1).start()

    def prefetch(t):
        g, kh = t // 2, lax.rem(t, 2)

        @pl.when(t < 2 * RING_GROUPS)
        def _():
            qkv_copy(0, kh, g, 6 * g + kh).start()
            qkv_copy(1, kh, g, 6 * g + 2 + kh).start()

        @pl.when(t < 2 * RING_GROUPS - 1)
        def _():
            qkv_copy(2, kh, g, 6 * g + 4 + kh).start()

    def piece(k):
        return pl.ds(pl.multiple_of(k * PIECE, PIECE), PIECE)

    def z_copy(k):
        return remote(
            abuf.at[pl.ds(core * n_grp, n_out), piece(k)], ybuf.at[pl.ds(core * n_out, n_out), piece(k)],
            zsnd.at[k], zrcv.at[k], {"pp": nxt})

    def z_tail(h):
        at, n = n_piece - 1 + h, n_out // 2
        return remote(
            abuf.at[pl.ds(core * n_grp + h * n, n), piece(n_piece - 1)],
            ybuf.at[pl.ds(core * n_out + h * n, n), piece(n_piece - 1)], zsnd.at[at], zrcv.at[at], {"pp": nxt})

    def fwd_copy(k):
        half_rows = ybuf.at[pl.ds(core * n_out, n_out), piece(k)]
        return remote(half_rows, half_rows, fsend.at[k], frcv.at[k], {"ep": partner})

    def round_rows(k, blocks):
        near = pl.ds(pl.multiple_of(chip * tok_chip + k * PIECE, PIECE), PIECE)
        for b in blocks:
            cols = slice(b * gw, (b + 1) * gw)
            abuf[core * n_grp + b, piece(k), :] = (pkeep[near, cols] + yrecv[piece(k), cols]).astype(BF16)

    def step_y(k):
        if isinstance(k, int) and k == n_piece - 1:
            for h in range(2):
                y_tail(h).wait_recv()
                round_rows(k, range(h * n_out // 2, (h + 1) * n_out // 2))
                z_tail(h).start()
            return
        if isinstance(k, int) and k >= n_piece - 2:
            y_copy(k, 1).wait_recv()
        else:
            @pl.when(lax.rem(k, 2) == 0)
            def _():
                y_copy(k, 2).wait_recv()
        round_rows(k, range(n_out))
        z_copy(k).start()

    def step_z(k):
        if isinstance(k, int) and k == n_piece - 1:
            z_tail(0).wait_recv()
            z_tail(1).wait_recv()
        else:
            z_copy(k).wait_recv()
        fwd_copy(k).start()

    def step_norm(k):
        fwd_copy(k).wait_recv()
        rows = piece(k)
        sq = None
        for b in range(2 * n_out):
            val = ybuf[b, rows, :].astype(F32)
            term = jnp.sum(val * val, axis=-1, keepdims=True)
            sq = term if sq is None else sq + term
        inv = lax.rsqrt(sq / float(d_model) + NORM_EPS)
        for b in range(2 * n_out):
            cols = slice(b * gw, (b + 1) * gw)
            xbuf[rows, cols] = (ybuf[b, rows, :].astype(F32) * inv * nw_ref[:, cols]).astype(BF16)

    z_lag, f_lag, first_z = 4, 6, 2

    g_blk = core * n_grp + n_out
    gcol = min(256, gw)

    def chunk(s, carry):
        row0 = chunk_row(s)
        rows = pl.ds(row0, ROWS)
        here = mp[rows, :]
        shift = (me * exp_rows).astype(F32)
        target = here[:, 0:8] + here[:, 16:24] + here[:, 32:40] - shift
        for cb in range(exp_rows // 256):
            col = lax.broadcasted_iota(jnp.int32, (ROWS, 256), 1).astype(F32) + float(cb * 256)
            g0 = jnp.zeros((ROWS, 256), F32)
            g1 = jnp.zeros((ROWS, 256), F32)
            g2 = jnp.zeros((ROWS, 256), F32)
            for j in range(8):
                hit = col == target[:, j:j + 1]
                g0 = jnp.where(hit, here[:, 8 + j:9 + j], g0)
                g1 = jnp.where(hit, here[:, 24 + j:25 + j], g1)
                g2 = jnp.where(hit, here[:, 40 + j:41 + j], g2)
            for part, val in enumerate((g0, g1, g2)):
                for c0 in range(0, 256, gcol):
                    at = cb * 256 + c0
                    abuf[g_blk + at // gw, part * ROWS:(part + 1) * ROWS, at % gw:at % gw + gcol] = val[:, c0:c0 + gcol].astype(BF16)
        lane_h = lax.broadcasted_iota(jnp.int32, (ROWS, LANES), 1).astype(F32)
        is_mine = (tok[rows, :] - (me * tok_dev).astype(F32) == lane_h) & (lane_h < float(tok_dev))
        pick = jnp.where(is_mine, 1.0, 0.0).astype(BF16)[:, :tok_dev]
        @pl.when(s >= 1)
        def _():
            pair_copy(s - 1).wait_send()

        for side in range(2):
            hh = (1 - core) if side == 0 else core
            for q in range(4):
                o_cols = wbuf[o_slot + 2 * hh + q // 2, (q % 2) * exp_rows:(q % 2 + 1) * exp_rows, :]
                h_cols = abuf[(1 - core) * n_grp + hh * n_out + q, 0:tok_dev, :]
                p3 = None
                for kb in range(exp_rows // gw):
                    term = mm(abuf[g_blk + kb, 0:3 * ROWS, :], o_cols[kb * gw:(kb + 1) * gw, :])
                    p3 = term if p3 is None else p3 + term
                total = p3[0:ROWS] + p3[ROWS:2 * ROWS] + p3[2 * ROWS:3 * ROWS] + mm(pick, h_cols)
                if side == 0:
                    pout[:, q * gw:(q + 1) * gw] = total
                else:
                    pkeep[rows, q * gw:(q + 1) * gw] = total
            if side == 0:
                pair_copy(s).start()
                prefetch(s + 2)

        finish(s)
        for lag, step in ((first_z, step_y), (first_z + z_lag, step_z), (first_z + f_lag, step_norm)):
            @pl.when(s >= lag)
            def _():
                step(s - lag)
        return carry

    lax.fori_loop(0, 2 * n_chunk, chunk, 0)
    for t in range(o_slot, SLOTS):
        qkv_copy(t % 6 // 2, t % 2, t // 6, t).start()
    for k in range(2 * n_chunk - first_z, n_piece + f_lag):
        if k < n_piece:
            step_y(k)
        if z_lag <= k < n_piece + z_lag:
            step_z(k - z_lag)
        if k >= f_lag:
            step_norm(k - f_lag)

    def a_copy(g):
        return remote(abuf.at[core * n_grp + g], abuf.at[core * n_grp + g], asend.at[g], arcv.at[g], {"ep": partner})

    r_id = lax.broadcasted_iota(jnp.int32, (tok_chip, tok_chip), 0)
    c_id = lax.broadcasted_iota(jnp.int32, (tok_chip, tok_chip), 1)
    mask = (r_id // SEQ == c_id // SEQ) & (c_id <= r_id)

    n_head = gw // HEAD_DIM
    head = [slice(hd * HEAD_DIM, (hd + 1) * HEAD_DIM) for hd in range(n_head)]

    def slot_of(g, j):
        return lax.rem(6 * g + j, SLOTS)

    def project(m, g):
        acc = mm(xbuf[:, 0:slot_rows], wbuf[slot_of(g, 2 * m)]) + mm(xbuf[:, slot_rows:2 * slot_rows], wbuf[slot_of(g, 2 * m + 1)])
        return acc.astype(BF16)

    def scores(hd):
        return mm_t(qbuf[:, head[hd]], kbuf[:, head[hd]]) * (HEAD_DIM ** -0.5)

    def softmax(s):
        s = jnp.where(mask, s, -1e30)
        ex = jnp.exp(s - jnp.max(s, axis=-1, keepdims=True))
        return (ex / jnp.sum(ex, axis=-1, keepdims=True)).astype(BF16)

    def mix(g, hd, prob):
        abuf[core * n_grp + g, :, head[hd]] = mm(prob, vbuf[:, head[hd]]).astype(BF16)

    def refill(g, j):
        ahead = j + SLOTS
        g2, j2 = g + ahead // 6, ahead % 6

        @pl.when(g2 < n_grp)
        def _():
            qkv_copy(j2 // 2, j2 % 2, g2, slot_of(g, j)).start()

        w = 6 * (g2 - n_grp) + j2

        @pl.when((w >= 0) & (w < 4 * n_out))
        def _():
            wo_copy(w).start()

    def wait_group(g):
        for j in range(6):
            qkv_copy(j // 2, j % 2, g, slot_of(g, j)).wait()

    for k in range(n_piece - 1):
        z_copy(k).wait_send()
    for h in range(2):
        z_tail(h).wait_send()
    wait_group(0)
    for m, buf in enumerate((qbuf, kbuf, vbuf)):
        buf[...] = project(m, 0)
        refill(0, 2 * m)
        refill(0, 2 * m + 1)

    def group(g, carry):
        wait_group(g)
        raw = [scores(hd) for hd in range(n_head)]
        q_new = project(0, g)
        probs = [softmax(raw[hd]) for hd in range(n_head)]
        qbuf[...] = q_new
        k_new = project(1, g)
        kbuf[...] = k_new
        for hd in range(n_head):
            mix(g - 1, hd, probs[hd])
        v_new = project(2, g)
        vbuf[...] = v_new
        a_copy(g - 1).start()
        for j in range(6):
            refill(g, j)
        return carry

    lax.fori_loop(1, n_grp, group, 0)
    last = n_grp - 1
    for hd, prob in enumerate([softmax(scores(hd)) for hd in range(n_head)]):
        mix(last, hd, prob)
    a_copy(last).start()

    for g in range(n_grp):
        a_copy(g).wait_recv()

    def out_cols(n):
        return pl.ds(pl.multiple_of(core * half + n * gw, gw), gw)

    def z_cols(n):
        return pl.ds(pl.multiple_of(n * gw, gw), gw)

    def out_remote(n):
        rows = pl.ds(pl.multiple_of((1 - core) * tok_dev, tok_dev), tok_dev)
        return remote(xbuf.at[rows, z_cols(n)], z_ref.at[:, out_cols(n)], outs.at[n], outr.at[n], {"ep": partner})

    def out_part(n, kq):
        slot = lax.rem(6 * n_grp + 4 * n + kq, SLOTS)
        acc = None
        for gg in range(grp_per_slot):
            term = mm(abuf[kq * grp_per_slot + gg], wbuf[slot, gg * gw:(gg + 1) * gw, :])
            acc = term if acc is None else acc + term
        return acc

    def out_done(n, acc):
        resid = ybuf[core * n_out + n].astype(F32)
        xbuf[:, z_cols(n)] = (resid + acc.astype(BF16).astype(F32)).astype(BF16)
        out_remote(n).start()
        mine = pl.ds(pl.multiple_of(core * tok_dev, tok_dev), tok_dev)
        z_ref[:, out_cols(n)] = xbuf[mine, z_cols(n)]

    def out_group(n, carry):
        for kq in range(4):
            wo_copy(4 * n + kq).wait()
        out_done(n, out_part(n, 0) + out_part(n, 1) + out_part(n, 2) + out_part(n, 3))
        return carry

    lax.fori_loop(0, n_out - 1, out_group, 0)
    end = n_out - 1
    total = None
    for kq in range(4):
        wo_copy(4 * end + kq).wait()
        part = out_part(end, kq)
        total = part if total is None else total + part
    out_done(end, total)

    own_copy.wait_send()
    for cp in meta_copies:
        cp.wait_send()
    pair_copy(2 * n_chunk - 1).wait_send()
    for f in range(n_chunk - 1):
        y_copy(2 * f, 2).wait_send()
    y_copy(n_piece - 2, 1).wait_send()
    for h in range(2):
        y_tail(h).wait_send()
    for k in range(n_piece):
        fwd_copy(k).wait_send()
    for g in range(n_grp):
        a_copy(g).wait_send()
    for n in range(n_out):
        out_remote(n).wait()


def solution(mesh):
    n_pp = mesh.shape['pp']
    group_axes = ('data', 'pp')

    def device_step(expert_out, expert_id, slot_id, gate, resid, owner, norm_w, w_q, w_k, w_v, w_o):
        d_model = resid.shape[3]
        tok_dev = resid.shape[2]
        n_exp, cap = expert_out.shape[2], expert_out.shape[3]
        exp_rows = n_exp * cap
        width = w_q.shape[2]
        gw = d_model // 8
        n_grp = width // 2 // gw
        n_out = d_model // 2 // gw
        tok_chip = 2 * tok_dev
        half = d_model // 2
        anym = pl.BlockSpec(memory_space=pl.ANY)
        dma = pltpu.SemaphoreType.DMA
        n_chunk2 = 2 * tok_chip // ROWS
        n_piece = tok_chip // PIECE
        out = pl.pallas_call(
            functools.partial(stage_kernel, n_pp, gw, exp_rows, cap),
            out_shape=pltpu.VMEM((tok_dev, d_model), BF16),
            in_specs=[anym] * 11,
            out_specs=pl.BlockSpec(memory_space=pltpu.VMEM),
            scratch_shapes=[
                pltpu.VMEM((8, tok_dev), jnp.int32),
                pltpu.VMEM((8, tok_dev), jnp.int32),
                pltpu.VMEM((8, tok_dev), F32),
                pltpu.VMEM((1, owner.shape[1]), jnp.int32),
                pltpu.VMEM((1, d_model), F32),
                dma((5,)),
                pltpu.VMEM((SLOTS, d_model // 2, gw), BF16),
                pltpu.VMEM((4 * tok_dev, half), F32),
                pltpu.VMEM((ROWS, half), F32),
                pltpu.VMEM((2, ROWS, half), F32),
                pltpu.VMEM((tok_chip, half), F32),
                pltpu.VMEM((2 * n_out, tok_chip, gw), BF16),
                pltpu.VMEM((tok_chip, d_model), BF16),
                pltpu.VMEM((tok_chip, gw), BF16),
                pltpu.VMEM((tok_chip, gw), BF16),
                pltpu.VMEM((tok_chip, gw), BF16),
                pltpu.VMEM((2 * n_grp, tok_chip, gw), BF16),
                pltpu.VMEM((N_EP, 16, LANES), F32),
                pltpu.VMEM((4 * SEQ, LANES), F32),
                pltpu.VMEM((4 * tok_dev, LANES), F32),
                pltpu.VMEM((4 * tok_dev, LANES), F32),
                dma((SLOTS,)), dma((8,)), dma((8,)),
                dma((3,)), dma((3,)), dma, dma,
                dma((n_chunk2,)), dma((n_chunk2,)),
                dma((n_piece + 1,)), dma((n_piece + 1,)),
                dma((n_piece + 1,)), dma((n_piece + 1,)),
                dma((n_piece,)), dma((n_piece,)),
                dma((n_grp,)), dma((n_grp,)),
                dma((n_out,)), dma((n_out,)),
            ],
            compiler_params=pltpu.CompilerParams(
                collective_id=0, has_side_effects=True, vmem_limit_bytes=66519040),
        )(expert_id[0, 0].T, slot_id[0, 0].T, gate[0, 0].T, owner, norm_w, expert_out.reshape(exp_rows, d_model), resid.reshape(tok_dev, d_model),
          w_q[0], w_k[0], w_v[0], w_o[0])
        return out.reshape(1, 1, tok_dev, d_model)

    tok_spec = P(group_axes, None, 'ep', None)
    weight_spec = P('pp', None, None)
    in_specs = (P(group_axes, None, 'ep', None, None), tok_spec, tok_spec, tok_spec, tok_spec, P(group_axes, None), P('pp', None), weight_spec, weight_spec, weight_spec, weight_spec)
    return jax.shard_map(device_step, mesh=mesh, in_specs=in_specs, out_specs=tok_spec, check_vma=False)
```
